32 devices in a mesh: slab: 8 (over z, y), energy: 4 (over x, core).
Axes of the slice: x: 2, y: 2, z: 4, core: 2. Of those that a mesh axis runs over, the one named last changes fastest.
Arguments:
- green: bfloat16 [4, 8, 3, 2, 384, 384], P('energy', 'slab'), may hold values from -0.3125 to 0.3125
- sigma: bfloat16 [4, 8, 3, 2, 384, 384], P('energy', 'slab'), may hold values from -4 to 4
- phonon: bfloat16 [4, 8, 2, 384, 384], P('energy', 'slab'), may hold values from -4 to 4
- pair_off: int32 [8, 3], replicated, may hold values from -2 to 2, as said below
- pair_count: int32 [8], replicated, may hold values from 1 to 3, as said below
- pair_range: int32 [8, 3], replicated, may hold values from 96 to 384, as said below
Outputs:
- lesser: float32 [4, 8, 2, 384, 384], P('energy', 'slab')
The draws below stay inside these ranges and needn't reach their ends.
Inputs may be any that keep to these rules, and one draw needn't show every extreme that they name: The partner slab k + pair_off[k, q] lies inside the grid. `pair_count`: some slab has 3 live slots. `pair_range`: a multiple of 96; some pair couples all 384 orbitals.
All inputs are finite; a program needn't handle non-finite values.
Results may differ from the reference program's by a relative error of at most 0.0035.
Values may be sent and summed in bfloat16 or wider, within the bound.
A program may use at most 64 MiB of HBM per device.

```python
import jax
import jax.numpy as jnp
from jax import lax

ORB = 384
MAXP = 3
NSLAB = 8
EN = 4


def draw_pair_off(key, part):
    shifts = jax.random.randint(key, (NSLAB, MAXP), -2, 3).astype(jnp.int32)
    slab_ids = jnp.arange(NSLAB, dtype=jnp.int32)[:, None]
    partner = slab_ids + shifts
    outside = (partner < 0) | (partner >= NSLAB)
    return jnp.where(outside, -shifts, shifts).astype(jnp.int32)


def draw_pair_count(key, part):
    counts = jax.random.randint(jax.random.fold_in(key, 11), (NSLAB,), 1, MAXP + 1).astype(jnp.int32)
    fullest = jax.random.randint(jax.random.fold_in(key, 12), (), 0, NSLAB)
    return counts.at[fullest].set(MAXP).astype(jnp.int32)


def draw_pair_range(key, part):
    quarters = jax.random.randint(jax.random.fold_in(key, 21), (NSLAB, MAXP), 1, 5).astype(jnp.int32)
    widest = jax.random.randint(jax.random.fold_in(key, 22), (), 0, NSLAB)
    quarters = quarters.at[widest, 0].set(4)
    return (quarters * (ORB // 4)).astype(jnp.int32)


def block_levels(own_key, dims, split, low, largest):
    loudness = 1.0
    for dim, parts in split:
        heights = jax.random.uniform(jax.random.fold_in(jax.random.fold_in(own_key, 6), dim), (parts,), jnp.float32, low / len(split), largest / len(split))
        loudness = loudness * jnp.repeat(jnp.exp(heights), dims[dim] // parts).reshape((-1,) + (1,) * (len(dims) - 1 - dim))
    return loudness


def bell_draw(own_key, shape, spread, most, pieces=(), kind=jnp.bfloat16):
    entries = jax.random.normal(own_key, shape, jnp.float32) * spread
    if len(pieces) > 0:
        entries = block_levels(own_key, shape, pieces, -0.22, 0.18) * entries
    return jnp.clip(entries, min=-most, max=most).astype(kind)


def setup_inputs(seed: int = 0) -> dict:
    keys = jax.random.split(jax.random.key(seed), 7)
    green = bell_draw(keys[0], (EN, NSLAB, 3, 2, ORB, ORB), ORB ** -0.5, 0.3125, ((0, 4), (1, 8)))
    sigma = bell_draw(keys[1], (EN, NSLAB, MAXP, 2, ORB, ORB), 0.3, 4.0, ((0, 4), (1, 8)))
    phonon = bell_draw(keys[2], (EN, NSLAB, 2, ORB, ORB), 0.3, 4.0, ((0, 4), (1, 8)))
    pair_off = draw_pair_off(jax.random.fold_in(keys[6], 71), 0)
    pair_count = draw_pair_count(jax.random.fold_in(keys[6], 71), 0)
    pair_range = draw_pair_range(jax.random.fold_in(keys[6], 71), 0)
    return {"green": green, "sigma": sigma, "phonon": phonon, "pair_off": pair_off, "pair_count": pair_count, "pair_range": pair_range}


def conj_sum(source, chosen):
    real = jnp.einsum('qmn,qpn->mp', source[:, 0], chosen[:, 0]) + jnp.einsum('qmn,qpn->mp', source[:, 1], chosen[:, 1])
    imag = jnp.einsum('qmn,qpn->mp', source[:, 1], chosen[:, 0]) - jnp.einsum('qmn,qpn->mp', source[:, 0], chosen[:, 1])
    return real, imag


def complex_times(left, real, imag):
    first = jnp.dot(left[0], real, preferred_element_type=jnp.float32) - jnp.dot(left[1], imag, preferred_element_type=jnp.float32)
    second = jnp.dot(left[0], imag, preferred_element_type=jnp.float32) + jnp.dot(left[1], real, preferred_element_type=jnp.float32)
    return jnp.stack([first, second])


def reference(green, sigma, phonon, pair_off, pair_count, pair_range):
    slab_total = green.shape[1]
    width = green.shape[-1]
    slots = pair_off.shape[1]
    positions = jnp.arange(width, dtype=jnp.int32)
    inside = positions[None, None, :] < pair_range[:, :, None]
    square = inside[:, :, :, None] & inside[:, :, None, :]
    masked = jnp.where(square[None, :, :, None], sigma, jnp.zeros((), jnp.bfloat16))
    padded = jnp.pad(phonon.astype(jnp.float32), ((1, 1), (0, 0), (0, 0), (0, 0), (0, 0)))
    phonon_mix = (0.5 * (padded[:-2] + padded[2:])).astype(jnp.bfloat16)
    sources = jnp.concatenate([masked, phonon_mix[:, :, None]], axis=2)
    slot_ids = jnp.arange(slots, dtype=jnp.int32)

    def one_row(flat):
        energy = flat // slab_total
        slab = flat % slab_total
        green_row = green[energy, slab]
        running = jnp.zeros((2, width, width), jnp.float32)
        for delta in (-1, 0, 1):
            other = (slab + delta).astype(jnp.int32)
            clipped = jnp.clip(other, 0, slab_total - 1).astype(jnp.int32)
            valid = (other >= 0) & (other < slab_total)
            source = sources[energy, clipped].astype(jnp.float32)
            offsets = pair_off[clipped]
            count = pair_count[clipped]
            place = (clipped + offsets - slab + 1).astype(jnp.int32)
            usable = (place >= 0) & (place <= 2) & (slot_ids < count)
            pick = jnp.concatenate([jnp.clip(place, 0, 2).astype(jnp.int32), jnp.array([delta + 1], jnp.int32)])
            keep = jnp.concatenate([usable, jnp.array([True])]).astype(jnp.float32)
            chosen = green_row[pick].astype(jnp.float32) * keep[:, None, None, None]
            real, imag = conj_sum(source, chosen)
            term = complex_times(green_row[delta + 1], real.astype(jnp.bfloat16), imag.astype(jnp.bfloat16))
            running = running + jnp.where(valid, term, jnp.zeros_like(term))
        return running

    flat_ids = jnp.arange(green.shape[0] * slab_total, dtype=jnp.int32)
    result = lax.map(one_row, flat_ids)
    return result.reshape(green.shape[0], slab_total, 2, width, width)
```

```python
import functools

import jax
import jax.numpy as jnp
from jax import lax
from jax.experimental import pallas as pl
from jax.experimental.pallas import tpu as pltpu
from jax.sharding import PartitionSpec as P

STRIPS = 4
OFFSETS = (-2, -1, 1, 2)
LAG = 2
MESH = pl.DeviceIdType.MESH


def shapes(slots):
    most = STRIPS * min(slots, len(OFFSETS))
    reach = min(2 * STRIPS, most)
    table = [(4, 2, 2, 0), (5, 3, 2, 1), (6, 4, 3, 1), (7, 5, 3, 1), (8, 6, 4, 1), (10, 8, 4, 1)]
    return [c for c in table if c[0] < most] + [(most, max(most - LAG, reach), 2, 0)]


def plan(slabs, strip, classes, off_ref, count_ref, range_ref, which_ref, plan_ref):
    slots = off_ref.shape[0]
    levels = slabs // 2

    def count(k, carry):
        side = 1 - 2 * lax.rem(k, 2)
        for n, order in enumerate(OFFSETS):
            most = jnp.int32(0)
            for q in range(slots):
                used = (off_ref[q, k] == order * side) & (q < count_ref[k])
                most = jnp.maximum(most, jnp.where(used, (range_ref[q, k] + strip - 1) // strip, 0))
            plan_ref[k, n] = most
        for n in range(4, 8):
            plan_ref[k, n] = jnp.int32(0)
        return carry

    lax.fori_loop(0, slabs, count, 0)
    for k in (slabs, slabs + 1):
        for n in range(8):
            plan_ref[k, n] = jnp.int32(0)

    def slab_at(column, p):
        inside = 2 * p + 1 if column else slabs - 2 - 2 * p
        return jnp.where(p < levels, inside, slabs + column)

    def loads(column, p):
        k, ahead = slab_at(column, p), slab_at(column, p + 1)
        far = plan_ref[k, 0] + plan_ref[k, 1]
        near = plan_ref[k, 2] + plan_ref[k, 3]
        return k, ahead, far, near, plan_ref[ahead, 2] + plan_ref[ahead, 3]

    def lend(far, near, after, before, cls):
        slots_y, forwarded, most_ahead, most_back = cls
        return jnp.maximum(
            jnp.maximum(near + far + before - slots_y, far - forwarded),
            -jnp.minimum(after, most_back),
        )

    def level(p, carry):
        lent, good = carry
        lent, good = [list(column) for column in lent], list(good)
        for column in range(2):
            _, _, far, near, after = loads(column, p)
            for n, cls in enumerate(classes):
                moved = lend(far, near, after, lent[column][n], cls)
                good[n] = good[n] & jnp.where(moved <= jnp.minimum(far, cls[2]), 1, 0)
                lent[column][n] = moved
        return tuple(tuple(column) for column in lent), tuple(good)

    zero = jnp.int32(0)
    start = (
        tuple(tuple(zero for _ in classes) for _ in range(2)),
        tuple(jnp.int32(1) for _ in classes),
    )
    _, good = lax.fori_loop(0, levels, level, start)
    which = jnp.int32(len(classes) - 1)
    chosen = [jnp.int32(v) for v in classes[-1]]
    for n in reversed(range(len(classes) - 1)):
        fits = good[n] > 0
        which = jnp.where(fits, n, which)
        chosen = [jnp.where(fits, v, c) for v, c in zip(classes[n], chosen)]
    which_ref[0] = which

    def settle(p, carry):
        out = []
        for column in range(2):
            k, ahead, far, near, after = loads(column, p)
            moved = lend(far, near, after, carry[column], chosen)
            gives = jnp.maximum(moved, 0)
            takes = jnp.maximum(-moved, 0)
            plan_ref[k, 4] = gives
            plan_ref[ahead, 6] = gives
            plan_ref[ahead, 5] = takes
            plan_ref[k, 7] = takes
            out.append(moved)
        return tuple(out)

    lax.fori_loop(0, levels, settle, (zero, zero))


def kernel(
    slabs,
    energies,
    cls,
    plan_ref,
    off_ref,
    count_ref,
    range_ref,
    green_hbm,
    sigma_hbm,
    phonon_hbm,
    out_ref,
    green_v,
    sigma_v,
    own,
    inbox,
    ahead_box,
    back_box,
    sides,
    right,
    left,
    whole,
    total,
    inner,
    inner_strip,
    send_own,
    recv_own,
    send_far,
    recv_far,
    send_lent,
    recv_lent,
    send_side,
    recv_side,
    load_sem,
):
    slots_y, forwarded, lent_ahead, lent_back = cls
    free = slots_y - forwarded
    early = min(3, forwarded - lent_back - max(0, lent_ahead - free))
    moves = slots_y + STRIPS
    passed = forwarded + STRIPS
    lent = lent_ahead + lent_back
    i = lax.axis_index("slab")
    e = lax.axis_index("energy")
    slots = sigma_hbm.shape[0]
    width = green_v.shape[-1]
    strip = width // STRIPS
    step = 1 - 2 * lax.rem(i, 2)
    partner = i + step
    goes = (i + 2 * step >= 0) & (i + 2 * step < slabs)
    comes = (i - 2 * step >= 0) & (i - 2 * step < slabs)
    onward = lax.rem(i + 2 * step + slabs, slabs)
    source = lax.rem(i - 2 * step + slabs, slabs)
    up = lax.rem(e + 1, energies)
    down = lax.rem(e - 1 + energies, energies)

    def remote(src, dst, send, recv, target):
        return pltpu.make_async_remote_copy(
            src_ref=src,
            dst_ref=dst,
            send_sem=send,
            recv_sem=recv,
            device_id=target,
            device_id_type=MESH,
        )

    def own_copy(n):
        return remote(own.at[n], inbox.at[n], send_own.at[n], recv_own.at[n], {"slab": partner})

    def far_copy(n):
        return remote(
            inbox.at[n], inbox.at[moves + n], send_far.at[n], recv_far.at[n], {"slab": onward}
        )

    def ahead_copy(n):
        return remote(
            own.at[moves + n], ahead_box.at[n], send_lent.at[n], recv_lent.at[n], {"slab": source}
        )

    def back_copy(n):
        return remote(
            own.at[moves + lent_ahead + n],
            back_box.at[n],
            send_lent.at[lent_ahead + n],
            recv_lent.at[lent_ahead + n],
            {"slab": onward},
        )

    def side_copy(place, s, target):
        return remote(
            phonon_hbm.at[:, s],
            sides.at[place, s],
            send_side.at[place, s],
            recv_side.at[place, s],
            {"energy": target},
        )

    loads = [
        pltpu.make_async_copy(sigma_hbm, sigma_v, load_sem.at[0]),
        pltpu.make_async_copy(green_hbm, green_v, load_sem.at[1]),
    ]
    for load in loads:
        load.start()

    barrier = pltpu.get_barrier_semaphore()
    for target in (partner, onward, source):
        pl.semaphore_signal(barrier, inc=1, device_id={"slab": target}, device_id_type=MESH)
    for target in (up, down):
        pl.semaphore_signal(barrier, inc=1, device_id={"energy": target}, device_id_type=MESH)

    rows = lax.broadcasted_iota(jnp.int32, (strip, width), 0)
    cols = lax.broadcasted_iota(jnp.int32, (strip, width), 1)

    def item(k, t):
        side = 1 - 2 * lax.rem(k, 2)
        first = plan_ref[k, 0]
        second = first + plan_ref[k, 1]
        third = second + plan_ref[k, 2]
        offset = jnp.where(t < first, -2, jnp.where(t < second, -1, jnp.where(t < third, 1, 2)))
        base = jnp.where(
            t < first, 0, jnp.where(t < second, first, jnp.where(t < third, second, third))
        )
        return offset * side, jnp.clip(t - base, 0, STRIPS - 1)

    def slot(k, j):
        far = plan_ref[k, 0] + plan_ref[k, 1]
        near = plan_ref[k, 2] + plan_ref[k, 3]
        far_own = far - plan_ref[k, 4]
        near_own = near - plan_ref[k, 5]
        behind = plan_ref[k, 6]
        ahead = plan_ref[k, 7]
        behind_late = jnp.minimum(behind, free)
        near_late = jnp.minimum(near_own, free - behind_late)
        behind_first = behind - behind_late
        near_first = near_own - near_late
        ahead_at = forwarded - ahead
        behind_at = ahead_at - behind_first
        u = j - forwarded
        kind = jnp.int32(0)
        entry = jnp.int32(0)
        for here, what, value in (
            ((u < 0) & (j < far_own + near_first), 2, far + j - far_own),
            ((u < 0) & (j < far_own), 1, j),
            ((u < 0) & (j >= behind_at), 3, j - behind_at),
            ((u < 0) & (j >= ahead_at), 4, j - ahead_at),
            ((u >= 0) & (u < near_late + behind_late), 3, behind_first + u - near_late),
            ((u >= 0) & (u < near_late), 2, far + near_first + u),
        ):
            kind = jnp.where(here, what, kind)
            entry = jnp.where(here, value, entry)
        return kind, entry

    def merged(offset, at_row, part, value):
        furthest = jnp.maximum(rows + at_row * strip, cols)
        for q in range(slots):
            used = (off_ref[q, i] == offset) & (q < count_ref[i])
            reach = jnp.where(used, range_ref[q, i], 0)
            value += jnp.where(furthest < reach, sigma_v[q, part, at_row].astype(jnp.float32), 0.0)
        return value.astype(jnp.bfloat16)

    def fresh(offset, at_row, part):
        return merged(offset, at_row, part, jnp.zeros((strip, width), jnp.float32))

    loads[0].wait()

    def pack_first(t, carry):
        head = min(2, early)
        is_lent = (t >= head) & (t < head + lent)
        j = jnp.where(t < head, t, t - lent)
        kind, entry = slot(i, j)
        far = plan_ref[i, 0] + plan_ref[i, 1]
        given = t - head
        back = given - lent_ahead
        near = plan_ref[i, 2] + plan_ref[i, 3]
        lent_entry = jnp.where(
            back >= 0, far + near - plan_ref[i, 5] + back, far - plan_ref[i, 4] + given
        )
        lent_live = jnp.where(back >= 0, back < plan_ref[i, 5], given < plan_ref[i, 4])
        entry = jnp.where(is_lent, lent_entry, entry)
        live = (is_lent & lent_live) | (jnp.logical_not(is_lent) & ((kind == 1) | (kind == 2)))
        offset, at_row = item(i, entry)
        offset = jnp.where(live, offset, 9)
        into = jnp.where(is_lent, moves + given, j)

        def one(part, inside):
            own[into, part] = fresh(offset, at_row, part)
            return inside

        lax.fori_loop(0, 2, one, 0)

        @pl.when(t == 0)
        def _():
            pl.semaphore_wait(barrier, 5)

        @pl.when(jnp.logical_not(is_lent))
        def _():
            own_copy(j).start()

        @pl.when(is_lent & (back < 0) & comes)
        def _():
            ahead_copy(given).start()

        if lent_back:

            @pl.when(is_lent & (back >= 0) & goes)
            def _():
                back_copy(back).start()

        @pl.when(t == 0)
        def _():
            for s in range(STRIPS):

                @pl.when(e < energies - 1)
                def _():
                    side_copy(0, s, up).start()

                @pl.when(e > 0)
                def _():
                    side_copy(1, s, down).start()

        return carry

    lax.fori_loop(0, early + lent, pack_first, 0)

    def pack_late():
        @pl.when(goes)
        def _():
            for n in range(lent_ahead):
                ahead_copy(n).wait_recv()

        if lent_back:

            @pl.when(comes)
            def _():
                for n in range(lent_back):
                    back_copy(n).wait_recv()

        def one(j, carry):
            kind, entry = slot(i, j)
            offset, at_row = item(i, entry)
            offset = jnp.where((kind == 1) | (kind == 2), offset, 9)

            def half(part, inside):
                value = fresh(offset, at_row, part)
                value = jnp.where(
                    kind == 3, ahead_box[jnp.clip(entry, 0, lent_ahead - 1), part], value
                )
                if lent_back:
                    value = jnp.where(
                        kind == 4, back_box[jnp.clip(entry, 0, lent_back - 1), part], value
                    )
                own[j + STRIPS, part] = value
                return inside

            lax.fori_loop(0, 2, half, 0)
            own_copy(j + STRIPS).start()
            return carry

        lax.fori_loop(early, slots_y, one, 0)

    def pass_on(n):
        own_copy(n).wait_recv()

        @pl.when(goes & (n < passed))
        def _():
            far_copy(n).start()

    loads[1].wait()

    def arrange(place, carry):
        real = green_v[place, 0]
        imag = green_v[place, 1]
        for g in range(STRIPS):
            span = slice(g * strip, (g + 1) * strip)
            left[place, g] = jnp.concatenate([real[:, span], imag[:, span]], axis=1)
        real_t = real.T
        imag_t = imag.T
        right[place, :width, :width] = real_t
        right[place, width:, :width] = imag_t
        right[place, :width, width:] = -imag_t
        right[place, width:, width:] = real_t
        return carry

    lax.fori_loop(0, 3, arrange, 0)

    tile = 2 * width // 3

    def multiply(place):
        def one(n, carry):
            span = pl.ds(pl.multiple_of(n * tile, tile), tile)
            total[:, span] += jnp.dot(
                whole[...], right[place, :, span], preferred_element_type=jnp.float32
            )
            return carry

        lax.fori_loop(0, 3, one, 0)

    total[...] = jnp.zeros_like(total)

    def add_own(m, carry):
        for s in range(STRIPS):
            for part in range(2):
                whole[s * strip : (s + 1) * strip, part * width : (part + 1) * width] = fresh(
                    2 * m - 1, s, part
                )
        multiply(2 * m)
        return carry

    lax.fori_loop(0, 2, add_own, 0)

    def mix(s, carry):
        @pl.when(e > 0)
        def _():
            side_copy(0, s, up).wait_recv()

        @pl.when(e == 0)
        def _():
            sides[0, s] = jnp.zeros(sides.shape[2:], sides.dtype)

        @pl.when(e < energies - 1)
        def _():
            side_copy(1, s, down).wait_recv()

        @pl.when(e == energies - 1)
        def _():
            sides[1, s] = jnp.zeros(sides.shape[2:], sides.dtype)

        for part in range(2):
            mixed = 0.5 * (
                sides[0, s, part].astype(jnp.float32) + sides[1, s, part].astype(jnp.float32)
            )
            mixed = mixed.astype(jnp.bfloat16).astype(jnp.float32)
            own[early + s, part] = merged(0, s, part, mixed)
        own_copy(early + s).start()
        return carry

    lax.fori_loop(0, STRIPS, mix, 0)
    pass_on(0)

    for s in range(STRIPS):
        for part in range(2):
            whole[s * strip : (s + 1) * strip, part * width : (part + 1) * width] = own[
                early + s, part
            ]
    multiply(1)
    pass_on(1)
    mine = total[...].astype(jnp.bfloat16)
    inner[:width, :] = mine
    inner[width:, :width] = -mine[:, width:]
    inner[width:, width:] = mine[:, :width]
    both = jnp.concatenate([green_v[1, 0], green_v[1, 1]], axis=1)
    for part in range(2):
        out_ref[part] = jnp.dot(
            both, inner[:, part * width : (part + 1) * width], preferred_element_type=jnp.float32
        )

    other = i - step

    def handle(at, n, across):
        j = jnp.where(n < early, n, n - STRIPS)
        middle = (n >= early) & (n < early + STRIPS)
        k = jnp.clip(jnp.where(across, partner, other), 0, slabs - 1)
        kind, entry = slot(k, j)
        crossed = kind == jnp.where(across, 3, 4)
        direct = kind == jnp.where(across, 2, 1)
        k_from = jnp.clip(jnp.where(across, other, partner), 0, slabs - 1)
        far_from = plan_ref[k_from, 0] + plan_ref[k_from, 1]
        near_from = plan_ref[k_from, 2] + plan_ref[k_from, 3]
        entry_from = entry + jnp.where(
            across, far_from - plan_ref[k_from, 4], far_from + near_from - plan_ref[k_from, 5]
        )
        k_used = jnp.where(crossed & jnp.logical_not(middle), k_from, k)
        offset, at_row = item(k_used, jnp.where(crossed, entry_from, entry))
        offset = jnp.where(middle, 0, offset)
        at_row = jnp.where(middle, jnp.clip(n - early, 0, STRIPS - 1), at_row)
        valid = middle | crossed | direct
        place = jnp.clip(k_used + offset - i + 1, 0, 2)
        column = jnp.clip(k_used - i + 1, 0, 2)
        data = jnp.concatenate([inbox[at, 0], inbox[at, 1]], axis=1)
        value = jnp.dot(data, right[place], preferred_element_type=jnp.float32)
        value = jnp.where(valid, value, 0.0).astype(jnp.bfloat16)
        inner_strip[:strip, :] = value
        inner_strip[strip:, :width] = -value[:, width:]
        inner_strip[strip:, width:] = value[:, :width]
        for part in range(2):
            out_ref[part] += jnp.dot(
                left[column, at_row],
                inner_strip[:, part * width : (part + 1) * width],
                preferred_element_type=jnp.float32,
            )

    def event(t, carry):
        n = t // 2
        across = lax.rem(t, 2) == 1
        m = n - LAG

        @pl.when(across & (n >= 2))
        def _():
            pass_on(n)

        @pl.when(across & (n == 3))
        def _():
            pack_late()

        @pl.when(jnp.logical_not(across) & (m >= 0) & comes)
        def _():
            far_copy(m).wait_recv()

        @pl.when(across | ((m >= 0) & comes))
        def _():
            index = jnp.where(across, n, m)
            handle(jnp.where(across, n, jnp.maximum(moves + m, 0)), index, across)

        return carry

    lax.fori_loop(0, 2 * moves, event, 0)

    for n in range(moves - LAG, passed):

        @pl.when(comes)
        def _():
            far_copy(n).wait_recv()
            handle(moves + n, jnp.int32(n), jnp.bool_(False))

    def sent(n, carry):
        own_copy(n).wait_send()

        @pl.when(goes & (n < passed))
        def _():
            far_copy(n).wait_send()

        return carry

    lax.fori_loop(0, moves, sent, 0)

    @pl.when(comes)
    def _():
        for n in range(lent_ahead):
            ahead_copy(n).wait_send()

    if lent_back:

        @pl.when(goes)
        def _():
            for n in range(lent_back):
                back_copy(n).wait_send()

    for s in range(STRIPS):

        @pl.when(e < energies - 1)
        def _():
            side_copy(0, s, up).wait_send()

        @pl.when(e > 0)
        def _():
            side_copy(1, s, down).wait_send()


def body(slabs, energies, green, sigma, phonon, pair_off, pair_count, pair_range):
    width = green.shape[-1]
    slots = sigma.shape[2]
    strip = width // STRIPS
    hbm = pl.BlockSpec(memory_space=pl.ANY)
    smem = pl.BlockSpec(memory_space=pltpu.SMEM)
    classes = shapes(slots)
    block = (2, width, width)
    cut = (2, strip, width)
    tables = (pair_off.T, pair_count, pair_range.T)

    def run(n):
        cls = classes[n]
        slots_y, forwarded, lent_ahead, lent_back = cls
        moves = slots_y + STRIPS
        passed = forwarded + STRIPS
        lent = lent_ahead + lent_back
        return pl.pallas_call(
            functools.partial(kernel, slabs, energies, cls),
            out_shape=jax.ShapeDtypeStruct(block, jnp.float32),
            in_specs=[smem, smem, smem, smem, hbm, hbm, hbm],
            out_specs=pl.BlockSpec(memory_space=pltpu.VMEM),
            scratch_shapes=[
                pltpu.VMEM((3,) + block, jnp.bfloat16),
                pltpu.VMEM((slots, 2, STRIPS, strip, width), jnp.bfloat16),
                pltpu.VMEM((moves + lent,) + cut, jnp.bfloat16),
                pltpu.VMEM((moves + passed,) + cut, jnp.bfloat16),
                pltpu.VMEM((lent_ahead,) + cut, jnp.bfloat16),
                pltpu.VMEM((max(1, lent_back),) + cut, jnp.bfloat16),
                pltpu.VMEM((2, STRIPS) + cut, jnp.bfloat16),
                pltpu.VMEM((3, 2 * width, 2 * width), jnp.bfloat16),
                pltpu.VMEM((3, STRIPS, width, 2 * strip), jnp.bfloat16),
                pltpu.VMEM((width, 2 * width), jnp.bfloat16),
                pltpu.VMEM((width, 2 * width), jnp.float32),
                pltpu.VMEM((2 * width, 2 * width), jnp.bfloat16),
                pltpu.VMEM((2 * strip, 2 * width), jnp.bfloat16),
                pltpu.SemaphoreType.DMA((moves,)),
                pltpu.SemaphoreType.DMA((moves,)),
                pltpu.SemaphoreType.DMA((passed,)),
                pltpu.SemaphoreType.DMA((passed,)),
                pltpu.SemaphoreType.DMA((lent,)),
                pltpu.SemaphoreType.DMA((lent,)),
                pltpu.SemaphoreType.DMA((2, STRIPS)),
                pltpu.SemaphoreType.DMA((2, STRIPS)),
                pltpu.SemaphoreType.DMA((2,)),
            ],
            compiler_params=pltpu.CompilerParams(collective_id=n, has_side_effects=True),
        )

    which, table = pl.pallas_call(
        functools.partial(plan, slabs, strip, classes),
        out_shape=(
            jax.ShapeDtypeStruct((1,), jnp.int32),
            jax.ShapeDtypeStruct((slabs + 2, 8), jnp.int32),
        ),
        in_specs=[smem, smem, smem],
        out_specs=(smem, smem),
    )(*tables)
    result = lax.switch(
        which[0],
        [run(n) for n in range(len(classes))],
        table,
        *tables,
        green[0, 0],
        sigma[0, 0].reshape(slots, 2, STRIPS, strip, width),
        phonon[0, 0].reshape(2, STRIPS, strip, width),
    )
    return result[None, None]


def solution(mesh):
    in_specs = (
        P("energy", "slab", None, None, None, None),
        P("energy", "slab", None, None, None, None),
        P("energy", "slab", None, None, None),
        P(),
        P(),
        P(),
    )
    out_specs = P("energy", "slab", None, None, None)
    run = functools.partial(body, mesh.shape["slab"], mesh.shape["energy"])
    return jax.shard_map(run, mesh=mesh, in_specs=in_specs, out_specs=out_specs, check_vma=False)
```

```python
import functools

import jax
import jax.numpy as jnp
from jax import lax
from jax.experimental import pallas as pl
from jax.experimental.pallas import tpu as pltpu
from jax.sharding import PartitionSpec as P

STRIPS = 4
OFFSETS = (-2, -1, 1, 2)
LAG = 2
PAIRS = 8
GRANT = 36 * 2**20
MESH = pl.DeviceIdType.MESH


def shapes(slots):
    most = STRIPS * min(slots, len(OFFSETS))
    reach = min(2 * STRIPS, most)
    table = [(4, 2, 2, 0), (5, 3, 2, 1), (6, 4, 3, 1), (7, 5, 3, 1), (8, 6, 4, 1), (10, 8, 4, 1)]
    return [c for c in table if c[0] < most] + [(most, max(most - LAG, reach), 2, 0)]


def plan(
    slabs,
    strip,
    classes,
    off_hbm,
    count_hbm,
    range_hbm,
    sigma_hbm,
    phonon_hbm,
    which_ref,
    plan_ref,
    sigma_v,
    phonon_v,
    off_ref,
    count_ref,
    range_ref,
    table_sem,
    load_sem,
):
    pairs = ((off_hbm, off_ref), (count_hbm, count_ref), (range_hbm, range_ref))
    tables = [pltpu.make_async_copy(a, b, table_sem.at[n]) for n, (a, b) in enumerate(pairs)]
    blocks = ((sigma_hbm, sigma_v), (phonon_hbm, phonon_v))
    fetches = [pltpu.make_async_copy(a, b, load_sem.at[n]) for n, (a, b) in enumerate(blocks)]
    for fetch in tables + fetches:
        fetch.start()
    for fetch in tables:
        fetch.wait()
    slots = off_ref.shape[0]
    levels = slabs // 2

    def count(k, carry):
        side = 1 - 2 * lax.rem(k, 2)
        live_slots = count_ref[k]
        offsets, heights = [], []
        for q in range(slots):
            offset = jnp.where(q < live_slots, off_ref[q, k], 9)
            reach = range_ref[q, k]
            height = jnp.int32(0)
            for n in range(STRIPS):
                height = jnp.where(reach > n * strip, n + 1, height)
            plan_ref[k, PAIRS + q] = offset
            plan_ref[k, PAIRS + slots + q] = reach
            offsets.append(offset * side)
            heights.append(height)
        for n, order in enumerate(OFFSETS):
            most = jnp.int32(0)
            for offset, height in zip(offsets, heights):
                most = jnp.maximum(most, jnp.where(offset == order, height, 0))
            plan_ref[k, n] = most
        return carry

    lax.fori_loop(0, slabs, count, 0)
    for k in (slabs, slabs + 1):
        for n in range(PAIRS + 2 * slots):
            plan_ref[k, n] = jnp.int32(0)

    for k in (1, slabs - 2):
        for n in (5, 6):
            plan_ref[k, n] = jnp.int32(0)

    def slab_at(column, p):
        inside = 2 * p + 1 if column else slabs - 2 - 2 * p
        return jnp.where(p < levels, inside, slabs + column)

    def loads(column, p):
        k, ahead = slab_at(column, p), slab_at(column, p + 1)
        far = plan_ref[k, 0] + plan_ref[k, 1]
        near = plan_ref[k, 2] + plan_ref[k, 3]
        return k, ahead, far, near, plan_ref[ahead, 2] + plan_ref[ahead, 3]

    def lend(far, near, after, before, cls):
        slots_y, forwarded, most_ahead, most_back = cls
        return jnp.maximum(
            jnp.maximum(near + far + before - slots_y, far - forwarded),
            -jnp.minimum(after, most_back),
        )

    def level(p, carry):
        lent, good = carry
        lent, good = [list(column) for column in lent], list(good)
        for column in range(2):
            _, _, far, near, after = loads(column, p)
            for n, cls in enumerate(classes):
                moved = lend(far, near, after, lent[column][n], cls)
                good[n] = good[n] & jnp.where(moved <= jnp.minimum(far, cls[2]), 1, 0)
                lent[column][n] = moved
        return tuple(tuple(column) for column in lent), tuple(good)

    zero = jnp.int32(0)
    start = (
        tuple(tuple(zero for _ in classes) for _ in range(2)),
        tuple(jnp.int32(1) for _ in classes),
    )
    _, good = lax.fori_loop(0, levels, level, start)
    which = jnp.int32(len(classes) - 1)
    chosen = [jnp.int32(v) for v in classes[-1]]
    for n in reversed(range(len(classes) - 1)):
        fits = good[n] > 0
        which = jnp.where(fits, n, which)
        chosen = [jnp.where(fits, v, c) for v, c in zip(classes[n], chosen)]
    which_ref[0] = which

    def settle(p, carry):
        out = []
        for column in range(2):
            k, ahead, far, near, after = loads(column, p)
            moved = lend(far, near, after, carry[column], chosen)
            gives = jnp.maximum(moved, 0)
            takes = jnp.maximum(-moved, 0)
            plan_ref[k, 4] = gives
            plan_ref[ahead, 6] = gives
            plan_ref[ahead, 5] = takes
            plan_ref[k, 7] = takes
            out.append(moved)
        return tuple(out)

    lax.fori_loop(0, levels, settle, (zero, zero))
    for fetch in fetches:
        fetch.wait()


def kernel(
    slabs,
    energies,
    cls,
    plan_ref,
    green_hbm,
    sigma_v,
    phonon_v,
    out_ref,
    green_v,
    own,
    inbox,
    ahead_box,
    back_box,
    sides,
    right,
    left,
    whole,
    total,
    inner,
    inner_strip,
    send_own,
    recv_own,
    send_far,
    recv_far,
    send_lent,
    recv_lent,
    send_side,
    recv_side,
    load_sem,
):
    slots_y, forwarded, lent_ahead, lent_back = cls
    free = slots_y - forwarded
    early = min(3, forwarded - lent_back - max(0, lent_ahead - free))
    moves = slots_y + STRIPS
    passed = forwarded + STRIPS
    lent = lent_ahead + lent_back
    i = lax.axis_index("slab")
    e = lax.axis_index("energy")
    slots = sigma_v.shape[0]
    width = green_v.shape[-1]
    strip = width // STRIPS
    step = 1 - 2 * lax.rem(i, 2)
    partner = i + step
    goes = (i + 2 * step >= 0) & (i + 2 * step < slabs)
    comes = (i - 2 * step >= 0) & (i - 2 * step < slabs)
    onward = lax.rem(i + 2 * step + slabs, slabs)
    source = lax.rem(i - 2 * step + slabs, slabs)
    up = lax.rem(e + 1, energies)
    down = lax.rem(e - 1 + energies, energies)

    def remote(src, dst, send, recv, target):
        return pltpu.make_async_remote_copy(
            src_ref=src,
            dst_ref=dst,
            send_sem=send,
            recv_sem=recv,
            device_id=target,
            device_id_type=MESH,
        )

    def own_copy(n):
        return remote(own.at[n], inbox.at[n], send_own.at[n], recv_own.at[n], {"slab": partner})

    def far_copy(n):
        return remote(
            inbox.at[n], inbox.at[moves + n], send_far.at[n], recv_far.at[n], {"slab": onward}
        )

    def ahead_copy(n):
        return remote(
            own.at[moves + n], ahead_box.at[n], send_lent.at[n], recv_lent.at[n], {"slab": source}
        )

    def back_copy(n):
        return remote(
            own.at[moves + lent_ahead + n],
            back_box.at[n],
            send_lent.at[lent_ahead + n],
            recv_lent.at[lent_ahead + n],
            {"slab": onward},
        )

    def side_copy(place, s, target):
        return remote(
            phonon_v.at[:, s],
            sides.at[place, s],
            send_side.at[place, s],
            recv_side.at[place, s],
            {"energy": target},
        )

    load = pltpu.make_async_copy(green_hbm, green_v, load_sem)
    load.start()

    barrier = pltpu.get_barrier_semaphore()
    for target in (partner, onward, source):
        pl.semaphore_signal(barrier, inc=1, device_id={"slab": target}, device_id_type=MESH)
    for target in (up, down):
        pl.semaphore_signal(barrier, inc=1, device_id={"energy": target}, device_id_type=MESH)

    rows = lax.broadcasted_iota(jnp.int32, (strip, width), 0)
    cols = lax.broadcasted_iota(jnp.int32, (strip, width), 1)

    def item(k, t):
        side = 1 - 2 * lax.rem(k, 2)
        first = plan_ref[k, 0]
        second = first + plan_ref[k, 1]
        third = second + plan_ref[k, 2]
        offset = jnp.where(t < first, -2, jnp.where(t < second, -1, jnp.where(t < third, 1, 2)))
        base = jnp.where(
            t < first, 0, jnp.where(t < second, first, jnp.where(t < third, second, third))
        )
        return offset * side, jnp.clip(t - base, 0, STRIPS - 1)

    def slot(k, j):
        far = plan_ref[k, 0] + plan_ref[k, 1]
        near = plan_ref[k, 2] + plan_ref[k, 3]
        far_own = far - plan_ref[k, 4]
        near_own = near - plan_ref[k, 5]
        behind = plan_ref[k, 6]
        ahead = plan_ref[k, 7]
        behind_late = jnp.minimum(behind, free)
        near_late = jnp.minimum(near_own, free - behind_late)
        behind_first = behind - behind_late
        near_first = near_own - near_late
        ahead_at = forwarded - ahead
        behind_at = ahead_at - behind_first
        u = j - forwarded
        kind = jnp.int32(0)
        entry = jnp.int32(0)
        for here, what, value in (
            ((u < 0) & (j < far_own + near_first), 2, far + j - far_own),
            ((u < 0) & (j < far_own), 1, j),
            ((u < 0) & (j >= behind_at), 3, j - behind_at),
            ((u < 0) & (j >= ahead_at), 4, j - ahead_at),
            ((u >= 0) & (u < near_late + behind_late), 3, behind_first + u - near_late),
            ((u >= 0) & (u < near_late), 2, far + near_first + u),
        ):
            kind = jnp.where(here, what, kind)
            entry = jnp.where(here, value, entry)
        return kind, entry

    def merged(offset, at_row, part, value):
        furthest = jnp.maximum(rows + at_row * strip, cols)
        for q in range(slots):
            used = plan_ref[i, PAIRS + q] == offset
            reach = jnp.where(used, plan_ref[i, PAIRS + slots + q], 0)
            value += jnp.where(furthest < reach, sigma_v[q, part, at_row].astype(jnp.float32), 0.0)
        return value.astype(jnp.bfloat16)

    def fresh(offset, at_row, part):
        return merged(offset, at_row, part, jnp.zeros((strip, width), jnp.float32))

    def pack_first(t, carry):
        head = min(2, early)
        is_lent = (t >= head) & (t < head + lent)
        j = jnp.where(t < head, t, t - lent)
        kind, entry = slot(i, j)
        far = plan_ref[i, 0] + plan_ref[i, 1]
        given = t - head
        back = given - lent_ahead
        near = plan_ref[i, 2] + plan_ref[i, 3]
        lent_entry = jnp.where(
            back >= 0, far + near - plan_ref[i, 5] + back, far - plan_ref[i, 4] + given
        )
        lent_live = jnp.where(back >= 0, back < plan_ref[i, 5], given < plan_ref[i, 4])
        entry = jnp.where(is_lent, lent_entry, entry)
        live = (is_lent & lent_live) | (jnp.logical_not(is_lent) & ((kind == 1) | (kind == 2)))
        offset, at_row = item(i, entry)
        offset = jnp.where(live, offset, 8)
        into = jnp.where(is_lent, moves + given, j)

        def one(part, inside):
            own[into, part] = fresh(offset, at_row, part)
            return inside

        lax.fori_loop(0, 2, one, 0)

        @pl.when(t == 0)
        def _():
            pl.semaphore_wait(barrier, 5)

        @pl.when(jnp.logical_not(is_lent))
        def _():
            own_copy(j).start()

        @pl.when(is_lent & (back < 0) & comes)
        def _():
            ahead_copy(given).start()

        if lent_back:

            @pl.when(is_lent & (back >= 0) & goes)
            def _():
                back_copy(back).start()

        @pl.when(t == 0)
        def _():
            for s in range(STRIPS):

                @pl.when(e < energies - 1)
                def _():
                    side_copy(0, s, up).start()

                @pl.when(e > 0)
                def _():
                    side_copy(1, s, down).start()

        return carry

    lax.fori_loop(0, early + lent, pack_first, 0)

    def pack_late():
        @pl.when(goes)
        def _():
            for n in range(lent_ahead):
                ahead_copy(n).wait_recv()

        if lent_back:

            @pl.when(comes)
            def _():
                for n in range(lent_back):
                    back_copy(n).wait_recv()

        def one(j, carry):
            kind, entry = slot(i, j)
            offset, at_row = item(i, entry)
            offset = jnp.where((kind == 1) | (kind == 2), offset, 8)

            def half(part, inside):
                value = fresh(offset, at_row, part)
                value = jnp.where(
                    kind == 3, ahead_box[jnp.clip(entry, 0, lent_ahead - 1), part], value
                )
                if lent_back:
                    value = jnp.where(
                        kind == 4, back_box[jnp.clip(entry, 0, lent_back - 1), part], value
                    )
                own[j + STRIPS, part] = value
                return inside

            lax.fori_loop(0, 2, half, 0)
            own_copy(j + STRIPS).start()
            return carry

        lax.fori_loop(early, slots_y, one, 0)

    def pass_on(n):
        own_copy(n).wait_recv()

        @pl.when(goes & (n < passed))
        def _():
            far_copy(n).start()

    load.wait()

    def arrange(place, carry):
        real = green_v[place, 0]
        imag = green_v[place, 1]
        for g in range(STRIPS):
            span = slice(g * strip, (g + 1) * strip)
            left[place, g] = jnp.concatenate([real[:, span], imag[:, span]], axis=1)
        real_t = real.T
        imag_t = imag.T
        right[place, :width, :width] = real_t
        right[place, width:, :width] = imag_t
        right[place, :width, width:] = -imag_t
        right[place, width:, width:] = real_t
        return carry

    lax.fori_loop(0, 3, arrange, 0)

    tile = 2 * width // 3

    def multiply(place):
        def one(n, carry):
            span = pl.ds(pl.multiple_of(n * tile, tile), tile)
            total[:, span] += jnp.dot(
                whole[...], right[place, :, span], preferred_element_type=jnp.float32
            )
            return carry

        lax.fori_loop(0, 3, one, 0)

    total[...] = jnp.zeros_like(total)

    def add_own(m, carry):
        for s in range(STRIPS):
            for part in range(2):
                whole[s * strip : (s + 1) * strip, part * width : (part + 1) * width] = fresh(
                    2 * m - 1, s, part
                )
        multiply(2 * m)
        return carry

    lax.fori_loop(0, 2, add_own, 0)

    def mix(s, carry):
        @pl.when(e > 0)
        def _():
            side_copy(0, s, up).wait_recv()

        @pl.when(e == 0)
        def _():
            sides[0, s] = jnp.zeros(sides.shape[2:], sides.dtype)

        @pl.when(e < energies - 1)
        def _():
            side_copy(1, s, down).wait_recv()

        @pl.when(e == energies - 1)
        def _():
            sides[1, s] = jnp.zeros(sides.shape[2:], sides.dtype)

        for part in range(2):
            mixed = 0.5 * (
                sides[0, s, part].astype(jnp.float32) + sides[1, s, part].astype(jnp.float32)
            )
            mixed = mixed.astype(jnp.bfloat16).astype(jnp.float32)
            own[early + s, part] = merged(0, s, part, mixed)
        own_copy(early + s).start()

        @pl.when(s == 0)
        def _():
            pass_on(0)

        @pl.when(s == STRIPS - 2)
        def _():
            pass_on(1)

        return carry

    lax.fori_loop(0, STRIPS, mix, 0)

    for s in range(STRIPS):
        for part in range(2):
            whole[s * strip : (s + 1) * strip, part * width : (part + 1) * width] = own[
                early + s, part
            ]
    multiply(1)
    mine = total[...].astype(jnp.bfloat16)
    inner[:width, :] = mine
    inner[width:, :width] = -mine[:, width:]
    inner[width:, width:] = mine[:, :width]
    both = jnp.concatenate([green_v[1, 0], green_v[1, 1]], axis=1)
    for part in range(2):
        out_ref[part] = jnp.dot(
            both, inner[:, part * width : (part + 1) * width], preferred_element_type=jnp.float32
        )

    other = i - step

    def handle(at, n, across):
        j = jnp.where(n < early, n, n - STRIPS)
        middle = (n >= early) & (n < early + STRIPS)
        k = jnp.clip(jnp.where(across, partner, other), 0, slabs - 1)
        kind, entry = slot(k, j)
        crossed = kind == jnp.where(across, 3, 4)
        direct = kind == jnp.where(across, 2, 1)
        k_from = jnp.clip(jnp.where(across, other, partner), 0, slabs - 1)
        far_from = plan_ref[k_from, 0] + plan_ref[k_from, 1]
        near_from = plan_ref[k_from, 2] + plan_ref[k_from, 3]
        entry_from = entry + jnp.where(
            across, far_from - plan_ref[k_from, 4], far_from + near_from - plan_ref[k_from, 5]
        )
        k_used = jnp.where(crossed & jnp.logical_not(middle), k_from, k)
        offset, at_row = item(k_used, jnp.where(crossed, entry_from, entry))
        offset = jnp.where(middle, 0, offset)
        at_row = jnp.where(middle, jnp.clip(n - early, 0, STRIPS - 1), at_row)
        valid = middle | crossed | direct
        place = jnp.clip(k_used + offset - i + 1, 0, 2)
        column = jnp.clip(k_used - i + 1, 0, 2)
        data = jnp.concatenate([inbox[at, 0], inbox[at, 1]], axis=1)
        value = jnp.dot(data, right[place], preferred_element_type=jnp.float32)
        value = jnp.where(valid, value, 0.0).astype(jnp.bfloat16)
        inner_strip[:strip, :] = value
        inner_strip[strip:, :width] = -value[:, width:]
        inner_strip[strip:, width:] = value[:, :width]
        for part in range(2):
            out_ref[part] += jnp.dot(
                left[column, at_row],
                inner_strip[:, part * width : (part + 1) * width],
                preferred_element_type=jnp.float32,
            )

    def event(t, carry):
        n = t // 2
        across = lax.rem(t, 2) == 1
        m = n - LAG

        @pl.when(across & (n >= 2))
        def _():
            pass_on(n)

        @pl.when(across & (n == 3))
        def _():
            pack_late()

        @pl.when(jnp.logical_not(across) & (m >= 0) & comes)
        def _():
            far_copy(m).wait_recv()

        @pl.when(across | ((m >= 0) & comes))
        def _():
            index = jnp.where(across, n, m)
            handle(jnp.where(across, n, jnp.maximum(moves + m, 0)), index, across)

        return carry

    lax.fori_loop(0, 2 * moves, event, 0)

    for n in range(moves - LAG, passed):

        @pl.when(comes)
        def _():
            far_copy(n).wait_recv()
            handle(moves + n, jnp.int32(n), jnp.bool_(False))

    def sent(n, carry):
        own_copy(n).wait_send()

        @pl.when(goes & (n < passed))
        def _():
            far_copy(n).wait_send()

        return carry

    lax.fori_loop(0, moves, sent, 0)

    @pl.when(comes)
    def _():
        for n in range(lent_ahead):
            ahead_copy(n).wait_send()

    if lent_back:

        @pl.when(goes)
        def _():
            for n in range(lent_back):
                back_copy(n).wait_send()

    for s in range(STRIPS):

        @pl.when(e < energies - 1)
        def _():
            side_copy(0, s, up).wait_send()

        @pl.when(e > 0)
        def _():
            side_copy(1, s, down).wait_send()


def body(slabs, energies, green, sigma, phonon, pair_off, pair_count, pair_range):
    width = green.shape[-1]
    slots = sigma.shape[2]
    strip = width // STRIPS
    hbm = pl.BlockSpec(memory_space=pl.ANY)
    smem = pl.BlockSpec(memory_space=pltpu.SMEM)
    vmem = pl.BlockSpec(memory_space=pltpu.VMEM)
    classes = shapes(slots)
    block = (2, width, width)
    cut = (2, strip, width)

    def run(n):
        cls = classes[n]
        slots_y, forwarded, lent_ahead, lent_back = cls
        moves = slots_y + STRIPS
        passed = forwarded + STRIPS
        lent = lent_ahead + lent_back
        call = pl.pallas_call(
            functools.partial(kernel, slabs, energies, cls),
            out_shape=jax.ShapeDtypeStruct(block, jnp.float32),
            in_specs=[smem, hbm, vmem, vmem],
            out_specs=vmem,
            scratch_shapes=[
                pltpu.VMEM((3,) + block, jnp.bfloat16),
                pltpu.VMEM((moves + lent,) + cut, jnp.bfloat16),
                pltpu.VMEM((moves + passed,) + cut, jnp.bfloat16),
                pltpu.VMEM((lent_ahead,) + cut, jnp.bfloat16),
                pltpu.VMEM((max(1, lent_back),) + cut, jnp.bfloat16),
                pltpu.VMEM((2, STRIPS) + cut, jnp.bfloat16),
                pltpu.VMEM((3, 2 * width, 2 * width), jnp.bfloat16),
                pltpu.VMEM((3, STRIPS, width, 2 * strip), jnp.bfloat16),
                pltpu.VMEM((width, 2 * width), jnp.bfloat16),
                pltpu.VMEM((width, 2 * width), jnp.float32),
                pltpu.VMEM((2 * width, 2 * width), jnp.bfloat16),
                pltpu.VMEM((2 * strip, 2 * width), jnp.bfloat16),
                pltpu.SemaphoreType.DMA((moves,)),
                pltpu.SemaphoreType.DMA((moves,)),
                pltpu.SemaphoreType.DMA((passed,)),
                pltpu.SemaphoreType.DMA((passed,)),
                pltpu.SemaphoreType.DMA((lent,)),
                pltpu.SemaphoreType.DMA((lent,)),
                pltpu.SemaphoreType.DMA((2, STRIPS)),
                pltpu.SemaphoreType.DMA((2, STRIPS)),
                pltpu.SemaphoreType.DMA,
            ],
            compiler_params=pltpu.CompilerParams(
                collective_id=n, has_side_effects=True, vmem_limit_bytes=GRANT
            ),
        )

        def placed(table, green, sigma, phonon):
            green = pltpu.with_memory_space_constraint(green, pltpu.HBM)
            sigma = pltpu.with_memory_space_constraint(sigma, pltpu.VMEM)
            phonon = pltpu.with_memory_space_constraint(phonon, pltpu.VMEM)
            table = pltpu.with_memory_space_constraint(table, pltpu.SMEM)
            return call(table, green, sigma, phonon)

        return placed

    sigma = sigma[0, 0].reshape(slots, 2, STRIPS, strip, width)
    phonon = phonon[0, 0].reshape(2, STRIPS, strip, width)
    arrays = (pair_off.T, pair_count, pair_range.T, sigma, phonon)
    which, table, sigma, phonon = pl.pallas_call(
        functools.partial(plan, slabs, strip, classes),
        out_shape=(
            pltpu.SMEM((1,), jnp.int32),
            pltpu.SMEM((slabs + 2, PAIRS + 2 * slots), jnp.int32),
            pltpu.VMEM(sigma.shape, sigma.dtype),
            pltpu.VMEM(phonon.shape, phonon.dtype),
        ),
        in_specs=[hbm] * 5,
        out_specs=(smem, smem, vmem, vmem),
        scratch_shapes=[
            pltpu.SMEM((slots, slabs), jnp.int32),
            pltpu.SMEM((slabs,), jnp.int32),
            pltpu.SMEM((slots, slabs), jnp.int32),
            pltpu.SemaphoreType.DMA((3,)),
            pltpu.SemaphoreType.DMA((2,)),
        ],
        compiler_params=pltpu.CompilerParams(vmem_limit_bytes=GRANT),
    )(*[pltpu.with_memory_space_constraint(x, pltpu.HBM) for x in arrays])
    green = green[0, 0]
    result = lax.switch(
        which[0], [run(n) for n in range(len(classes))], table, green, sigma, phonon
    )
    return result[None, None]


def solution(mesh):
    in_specs = (
        P("energy", "slab", None, None, None, None),
        P("energy", "slab", None, None, None, None),
        P("energy", "slab", None, None, None),
        P(),
        P(),
        P(),
    )
    out_specs = P("energy", "slab", None, None, None)
    run = functools.partial(body, mesh.shape["slab"], mesh.shape["energy"])
    return jax.shard_map(run, mesh=mesh, in_specs=in_specs, out_specs=out_specs, check_vma=False)
```

```python
import functools

import jax
import jax.numpy as jnp
from jax import lax
from jax.experimental import pallas as pl
from jax.experimental.pallas import tpu as pltpu
from jax.sharding import PartitionSpec as P

STRIPS = 4
OFFSETS = (-2, -1, 1, 2)
LAG = 2
LENT = 4
PAIRS = 5
GRANT = 36 * 2**20
MESH = pl.DeviceIdType.MESH


def shapes(slots):
    most = STRIPS * min(slots, len(OFFSETS))
    reach = min(2 * STRIPS, most)
    table = [(m, m - LAG, 4, min(2, m - 4), 2) for m in (4, 5, 6, 7, 8, 10)]
    return [c for c in table if c[0] < most] + [(most, max(most - LAG, reach), 2, 0, 2)]


def plan(
    slabs,
    strip,
    classes,
    off_hbm,
    count_hbm,
    range_hbm,
    sigma_hbm,
    which_ref,
    plan_ref,
    sigma_v,
    off_ref,
    count_ref,
    range_ref,
    table_sem,
    load_sem,
):
    pairs = ((off_hbm, off_ref), (count_hbm, count_ref), (range_hbm, range_ref))
    tables = [pltpu.make_async_copy(a, b, table_sem.at[n]) for n, (a, b) in enumerate(pairs)]
    blocks = ((sigma_hbm, sigma_v),)
    fetches = [pltpu.make_async_copy(a, b, load_sem.at[n]) for n, (a, b) in enumerate(blocks)]
    for fetch in tables + fetches:
        fetch.start()
    for fetch in tables:
        fetch.wait()
    slots = off_ref.shape[0]
    levels = slabs // 2

    group = next(n for n in (4, 2, 1) if slabs % n == 0)

    def count(m, carry):
        for k in [m * group + n for n in range(group)]:
            side = 1 - 2 * lax.rem(k, 2)
            live_slots = count_ref[k]
            offsets, heights = [], []
            for q in range(slots):
                offset = jnp.where(q < live_slots, off_ref[q, k], 9)
                reach = range_ref[q, k]
                height = jnp.int32(0)
                for n in range(STRIPS):
                    height = jnp.where(reach > n * strip, n + 1, height)
                plan_ref[k, PAIRS + q] = offset
                plan_ref[k, PAIRS + slots + q] = reach
                offsets.append(offset * side)
                heights.append(height)
            for n, order in enumerate(OFFSETS):
                most = jnp.int32(0)
                for offset, height in zip(offsets, heights):
                    most = jnp.maximum(most, jnp.where(offset == order, height, 0))
                plan_ref[k, n] = most
        return carry

    lax.fori_loop(0, slabs // group, count, 0)
    plan_ref[slabs, LENT] = jnp.int32(0)

    chains = []
    for column in range(2):
        chain = [2 * p + 1 if column else slabs - 2 - 2 * p for p in range(levels)]
        far = [plan_ref[k, 0] + plan_ref[k, 1] for k in chain]
        near = [plan_ref[k, 2] + plan_ref[k, 3] for k in chain]
        chains.append((chain, far, near))

    def pick(table, n):
        value = jnp.int32(table[-1])
        for m, entry in enumerate(table[:-1]):
            value = jnp.where(n == m, entry, value)
        return value

    def attempt(state):
        n = state[0] + 1
        slots_y, forwarded, most_ahead, most_back, early = [pick(t, n) for t in zip(*classes)]
        free = slots_y - forwarded
        bad = jnp.int32(0)
        for chain, far, near in chains:
            moved = jnp.int32(0)
            for p, k in enumerate(chain):
                after = near[p + 1] if p + 1 < levels else 0
                behind = jnp.maximum(moved, 0)
                room = forwarded - early - jnp.maximum(behind - free, 0)
                need = jnp.maximum(near[p] + far[p] + moved - slots_y, far[p] - forwarded)
                pull = jnp.minimum(jnp.minimum(after, most_back), room)
                moved = jnp.maximum(need, -pull)
                bad = bad | jnp.where((moved > jnp.minimum(far[p], most_ahead)) | (room < 0), 1, 0)
                plan_ref[k, LENT] = moved
        return n, bad

    n, _ = lax.while_loop(lambda state: state[1] > 0, attempt, (jnp.int32(-1), jnp.int32(1)))
    which_ref[0] = n
    for fetch in fetches:
        fetch.wait()


def kernel(
    slabs,
    energies,
    cls,
    plan_ref,
    green_hbm,
    sigma_v,
    phonon_hbm,
    out_ref,
    green_v,
    own,
    inbox,
    ahead_box,
    back_box,
    sides,
    right,
    left,
    whole,
    total,
    inner,
    inner_strip,
    send_own,
    recv_own,
    send_far,
    recv_far,
    send_lent,
    recv_lent,
    send_side,
    recv_side,
    load_sem,
):
    slots_y, forwarded, lent_ahead, lent_back, early = cls
    free = slots_y - forwarded
    moves = slots_y + STRIPS
    passed = forwarded + STRIPS
    lent = lent_ahead + lent_back
    i = lax.axis_index("slab")
    e = lax.axis_index("energy")
    slots = sigma_v.shape[0]
    width = green_v.shape[-1]
    strip = width // STRIPS
    step = 1 - 2 * lax.rem(i, 2)
    partner = i + step
    goes = (i + 2 * step >= 0) & (i + 2 * step < slabs)
    comes = (i - 2 * step >= 0) & (i - 2 * step < slabs)
    onward = lax.rem(i + 2 * step + slabs, slabs)
    source = lax.rem(i - 2 * step + slabs, slabs)
    up = lax.rem(e + 1, energies)
    down = lax.rem(e - 1 + energies, energies)

    def remote(src, dst, send, recv, target):
        return pltpu.make_async_remote_copy(
            src_ref=src,
            dst_ref=dst,
            send_sem=send,
            recv_sem=recv,
            device_id=target,
            device_id_type=MESH,
        )

    def own_copy(n):
        return remote(own.at[n], inbox.at[n], send_own.at[n], recv_own.at[n], {"slab": partner})

    def far_copy(n):
        return remote(
            inbox.at[n], inbox.at[moves + n], send_far.at[n], recv_far.at[n], {"slab": onward}
        )

    def ahead_copy(n):
        return remote(
            own.at[moves + n], ahead_box.at[n], send_lent.at[n], recv_lent.at[n], {"slab": source}
        )

    def back_copy(n):
        return remote(
            own.at[moves + lent_ahead + n],
            back_box.at[n],
            send_lent.at[lent_ahead + n],
            recv_lent.at[lent_ahead + n],
            {"slab": onward},
        )

    def side_copy(place, s, target):
        return remote(
            phonon_hbm.at[:, s],
            sides.at[place, s],
            send_side.at[place, s],
            recv_side.at[place, s],
            {"energy": target},
        )

    load = pltpu.make_async_copy(green_hbm, green_v, load_sem)
    load.start()

    barrier = pltpu.get_barrier_semaphore()
    for target in (partner, onward, source):
        pl.semaphore_signal(barrier, inc=1, device_id={"slab": target}, device_id_type=MESH)
    for target in (up, down):
        pl.semaphore_signal(barrier, inc=1, device_id={"energy": target}, device_id_type=MESH)

    rows = lax.broadcasted_iota(jnp.int32, (strip, width), 0)
    cols = lax.broadcasted_iota(jnp.int32, (strip, width), 1)

    def item(k, t):
        side = 1 - 2 * lax.rem(k, 2)
        first = plan_ref[k, 0]
        second = first + plan_ref[k, 1]
        third = second + plan_ref[k, 2]
        offset = jnp.where(t < first, -2, jnp.where(t < second, -1, jnp.where(t < third, 1, 2)))
        base = jnp.where(
            t < first, 0, jnp.where(t < second, first, jnp.where(t < third, second, third))
        )
        return offset * side, jnp.clip(t - base, 0, STRIPS - 1)

    def lending(k):
        before = k + 2 - 4 * lax.rem(k, 2)
        before = jnp.where((before >= 0) & (before < slabs), before, slabs)
        gives, takes = plan_ref[k, LENT], plan_ref[before, LENT]
        return (
            jnp.maximum(gives, 0),
            jnp.maximum(-takes, 0),
            jnp.maximum(takes, 0),
            jnp.maximum(-gives, 0),
        )

    def slot(k, j):
        far = plan_ref[k, 0] + plan_ref[k, 1]
        near = plan_ref[k, 2] + plan_ref[k, 3]
        lent_far, lent_near, behind, ahead = lending(k)
        far_own = far - lent_far
        near_own = near - lent_near
        behind_late = jnp.minimum(behind, free)
        near_late = jnp.minimum(near_own, free - behind_late)
        behind_first = behind - behind_late
        near_first = near_own - near_late
        ahead_at = forwarded - ahead
        behind_at = ahead_at - behind_first
        u = j - forwarded
        kind = jnp.int32(0)
        entry = jnp.int32(0)
        for here, what, value in (
            ((u < 0) & (j < far_own + near_first), 2, far + j - far_own),
            ((u < 0) & (j < far_own), 1, j),
            ((u < 0) & (j >= behind_at), 3, j - behind_at),
            ((u < 0) & (j >= ahead_at), 4, j - ahead_at),
            ((u >= 0) & (u < near_late + behind_late), 3, behind_first + u - near_late),
            ((u >= 0) & (u < near_late), 2, far + near_first + u),
        ):
            kind = jnp.where(here, what, kind)
            entry = jnp.where(here, value, entry)
        return kind, entry

    def merged(offset, at_row, part, value):
        furthest = jnp.maximum(rows + at_row * strip, cols)
        for q in range(slots):
            used = plan_ref[i, PAIRS + q] == offset
            reach = jnp.where(used, plan_ref[i, PAIRS + slots + q], 0)
            value += jnp.where(furthest < reach, sigma_v[q, part, at_row].astype(jnp.float32), 0.0)
        return value.astype(jnp.bfloat16)

    def fresh(offset, at_row, part):
        return merged(offset, at_row, part, jnp.zeros((strip, width), jnp.float32))

    def pack_first(t, carry):
        head = min(2, early)
        is_lent = (t >= head) & (t < head + lent)
        j = jnp.where(t < head, t, t - lent)
        kind, entry = slot(i, j)
        far = plan_ref[i, 0] + plan_ref[i, 1]
        given = t - head
        back = given - lent_ahead
        near = plan_ref[i, 2] + plan_ref[i, 3]
        lent_far, lent_near, _, _ = lending(i)
        lent_entry = jnp.where(back >= 0, far + near - lent_near + back, far - lent_far + given)
        lent_live = jnp.where(back >= 0, back < lent_near, given < lent_far)
        entry = jnp.where(is_lent, lent_entry, entry)
        live = (is_lent & lent_live) | (jnp.logical_not(is_lent) & ((kind == 1) | (kind == 2)))
        offset, at_row = item(i, entry)
        offset = jnp.where(live, offset, 8)
        into = jnp.where(is_lent, moves + given, j)

        def one(part, inside):
            own[into, part] = fresh(offset, at_row, part)
            return inside

        lax.fori_loop(0, 2, one, 0)

        @pl.when(t == 0)
        def _():
            pl.semaphore_wait(barrier, 5)

        @pl.when(jnp.logical_not(is_lent))
        def _():
            own_copy(j).start()

        @pl.when(is_lent & (back < 0) & comes)
        def _():
            ahead_copy(given).start()

        if lent_back:

            @pl.when(is_lent & (back >= 0) & goes)
            def _():
                back_copy(back).start()

        @pl.when(t == 0)
        def _():
            for s in range(STRIPS):

                @pl.when(e < energies - 1)
                def _():
                    side_copy(0, s, up).start()

                @pl.when(e > 0)
                def _():
                    side_copy(1, s, down).start()

        return carry

    lax.fori_loop(0, early + lent, pack_first, 0)

    def pack_late():
        @pl.when(goes)
        def _():
            for n in range(lent_ahead):
                ahead_copy(n).wait_recv()

        if lent_back:

            @pl.when(comes)
            def _():
                for n in range(lent_back):
                    back_copy(n).wait_recv()

        def one(j, carry):
            kind, entry = slot(i, j)
            offset, at_row = item(i, entry)
            offset = jnp.where((kind == 1) | (kind == 2), offset, 8)

            def half(part, inside):
                value = fresh(offset, at_row, part)
                value = jnp.where(
                    kind == 3, ahead_box[jnp.clip(entry, 0, lent_ahead - 1), part], value
                )
                if lent_back:
                    value = jnp.where(
                        kind == 4, back_box[jnp.clip(entry, 0, lent_back - 1), part], value
                    )
                own[j + STRIPS, part] = value
                return inside

            lax.fori_loop(0, 2, half, 0)
            own_copy(j + STRIPS).start()
            return carry

        lax.fori_loop(early, slots_y, one, 0)

    def pass_on(n):
        own_copy(n).wait_recv()

        @pl.when(goes & (n < passed))
        def _():
            far_copy(n).start()

    load.wait()

    def arrange(place, carry):
        real = green_v[place, 0]
        imag = green_v[place, 1]
        for g in range(STRIPS):
            span = slice(g * strip, (g + 1) * strip)
            left[place, g] = jnp.concatenate([real[:, span], imag[:, span]], axis=1)
        real_t = real.T
        imag_t = imag.T
        right[place, :width, :width] = real_t
        right[place, width:, :width] = imag_t
        right[place, :width, width:] = -imag_t
        right[place, width:, width:] = real_t
        return carry

    lax.fori_loop(0, 3, arrange, 0)

    tile = 2 * width // 3

    def multiply(place):
        def one(n, carry):
            span = pl.ds(pl.multiple_of(n * tile, tile), tile)
            total[:, span] += jnp.dot(
                whole[...], right[place, :, span], preferred_element_type=jnp.float32
            )
            return carry

        lax.fori_loop(0, 3, one, 0)

    total[...] = jnp.zeros_like(total)

    def add_own(m, carry):
        for s in range(STRIPS):
            for part in range(2):
                whole[s * strip : (s + 1) * strip, part * width : (part + 1) * width] = fresh(
                    2 * m - 1, s, part
                )
        multiply(2 * m)
        return carry

    lax.fori_loop(0, 2, add_own, 0)

    def mix(s, carry):
        @pl.when(e > 0)
        def _():
            side_copy(0, s, up).wait_recv()

        @pl.when(e == 0)
        def _():
            sides[0, s] = jnp.zeros(sides.shape[2:], sides.dtype)

        @pl.when(e < energies - 1)
        def _():
            side_copy(1, s, down).wait_recv()

        @pl.when(e == energies - 1)
        def _():
            sides[1, s] = jnp.zeros(sides.shape[2:], sides.dtype)

        for part in range(2):
            mixed = 0.5 * (
                sides[0, s, part].astype(jnp.float32) + sides[1, s, part].astype(jnp.float32)
            )
            mixed = mixed.astype(jnp.bfloat16).astype(jnp.float32)
            own[early + s, part] = merged(0, s, part, mixed)
        own_copy(early + s).start()

        @pl.when(s == 0)
        def _():
            pass_on(0)

        @pl.when(s == STRIPS - 2)
        def _():
            pass_on(1)

        return carry

    lax.fori_loop(0, STRIPS, mix, 0)

    for s in range(STRIPS):
        for part in range(2):
            whole[s * strip : (s + 1) * strip, part * width : (part + 1) * width] = own[
                early + s, part
            ]
    multiply(1)
    mine = total[...].astype(jnp.bfloat16)
    inner[:width, :] = mine
    inner[width:, :width] = -mine[:, width:]
    inner[width:, width:] = mine[:, :width]
    both = jnp.concatenate([green_v[1, 0], green_v[1, 1]], axis=1)
    for part in range(2):
        out_ref[part] = jnp.dot(
            both, inner[:, part * width : (part + 1) * width], preferred_element_type=jnp.float32
        )

    other = i - step

    def handle(at, n, across):
        j = jnp.where(n < early, n, n - STRIPS)
        middle = (n >= early) & (n < early + STRIPS)
        k = jnp.clip(jnp.where(across, partner, other), 0, slabs - 1)
        kind, entry = slot(k, j)
        crossed = kind == jnp.where(across, 3, 4)
        direct = kind == jnp.where(across, 2, 1)
        k_from = jnp.clip(jnp.where(across, other, partner), 0, slabs - 1)
        far_from = plan_ref[k_from, 0] + plan_ref[k_from, 1]
        near_from = plan_ref[k_from, 2] + plan_ref[k_from, 3]
        lent_far, lent_near, _, _ = lending(k_from)
        entry_from = entry + jnp.where(
            across, far_from - lent_far, far_from + near_from - lent_near
        )
        k_used = jnp.where(crossed & jnp.logical_not(middle), k_from, k)
        offset, at_row = item(k_used, jnp.where(crossed, entry_from, entry))
        offset = jnp.where(middle, 0, offset)
        at_row = jnp.where(middle, jnp.clip(n - early, 0, STRIPS - 1), at_row)
        valid = middle | crossed | direct
        place = jnp.clip(k_used + offset - i + 1, 0, 2)
        column = jnp.clip(k_used - i + 1, 0, 2)
        data = jnp.concatenate([inbox[at, 0], inbox[at, 1]], axis=1)
        value = jnp.dot(data, right[place], preferred_element_type=jnp.float32)
        value = jnp.where(valid, value, 0.0).astype(jnp.bfloat16)
        inner_strip[:strip, :] = value
        inner_strip[strip:, :width] = -value[:, width:]
        inner_strip[strip:, width:] = value[:, :width]
        for part in range(2):
            out_ref[part] += jnp.dot(
                left[column, at_row],
                inner_strip[:, part * width : (part + 1) * width],
                preferred_element_type=jnp.float32,
            )

    def event(t, carry):
        n = t // 2
        across = lax.rem(t, 2) == 1
        m = n - LAG

        @pl.when(across & (n >= 2))
        def _():
            pass_on(n)

        @pl.when(across & (n == 3))
        def _():
            pack_late()

        @pl.when(jnp.logical_not(across) & (m >= 0) & comes)
        def _():
            far_copy(m).wait_recv()

        @pl.when(across | ((m >= 0) & comes))
        def _():
            index = jnp.where(across, n, m)
            handle(jnp.where(across, n, jnp.maximum(moves + m, 0)), index, across)

        return carry

    lax.fori_loop(0, 2 * moves, event, 0)

    for n in range(moves - LAG, passed):

        @pl.when(comes)
        def _():
            far_copy(n).wait_recv()
            handle(moves + n, jnp.int32(n), jnp.bool_(False))

    def sent(n, carry):
        own_copy(n).wait_send()

        @pl.when(goes & (n < passed))
        def _():
            far_copy(n).wait_send()

        return carry

    lax.fori_loop(0, moves, sent, 0)

    @pl.when(comes)
    def _():
        for n in range(lent_ahead):
            ahead_copy(n).wait_send()

    if lent_back:

        @pl.when(goes)
        def _():
            for n in range(lent_back):
                back_copy(n).wait_send()

    for s in range(STRIPS):

        @pl.when(e < energies - 1)
        def _():
            side_copy(0, s, up).wait_send()

        @pl.when(e > 0)
        def _():
            side_copy(1, s, down).wait_send()


def body(slabs, energies, green, sigma, phonon, pair_off, pair_count, pair_range):
    width = green.shape[-1]
    slots = sigma.shape[2]
    strip = width // STRIPS
    hbm = pl.BlockSpec(memory_space=pl.ANY)
    smem = pl.BlockSpec(memory_space=pltpu.SMEM)
    vmem = pl.BlockSpec(memory_space=pltpu.VMEM)
    classes = shapes(slots)
    block = (2, width, width)
    cut = (2, strip, width)

    def run(n):
        cls = classes[n]
        slots_y, forwarded, lent_ahead, lent_back, _ = cls
        moves = slots_y + STRIPS
        passed = forwarded + STRIPS
        lent = lent_ahead + lent_back
        call = pl.pallas_call(
            functools.partial(kernel, slabs, energies, cls),
            out_shape=jax.ShapeDtypeStruct(block, jnp.float32),
            in_specs=[smem, hbm, vmem, hbm],
            out_specs=vmem,
            scratch_shapes=[
                pltpu.VMEM((3,) + block, jnp.bfloat16),
                pltpu.VMEM((moves + lent,) + cut, jnp.bfloat16),
                pltpu.VMEM((moves + passed,) + cut, jnp.bfloat16),
                pltpu.VMEM((lent_ahead,) + cut, jnp.bfloat16),
                pltpu.VMEM((max(1, lent_back),) + cut, jnp.bfloat16),
                pltpu.VMEM((2, STRIPS) + cut, jnp.bfloat16),
                pltpu.VMEM((3, 2 * width, 2 * width), jnp.bfloat16),
                pltpu.VMEM((3, STRIPS, width, 2 * strip), jnp.bfloat16),
                pltpu.VMEM((width, 2 * width), jnp.bfloat16),
                pltpu.VMEM((width, 2 * width), jnp.float32),
                pltpu.VMEM((2 * width, 2 * width), jnp.bfloat16),
                pltpu.VMEM((2 * strip, 2 * width), jnp.bfloat16),
                pltpu.SemaphoreType.DMA((moves,)),
                pltpu.SemaphoreType.DMA((moves,)),
                pltpu.SemaphoreType.DMA((passed,)),
                pltpu.SemaphoreType.DMA((passed,)),
                pltpu.SemaphoreType.DMA((lent,)),
                pltpu.SemaphoreType.DMA((lent,)),
                pltpu.SemaphoreType.DMA((2, STRIPS)),
                pltpu.SemaphoreType.DMA((2, STRIPS)),
                pltpu.SemaphoreType.DMA,
            ],
            compiler_params=pltpu.CompilerParams(
                collective_id=n, has_side_effects=True, vmem_limit_bytes=GRANT
            ),
        )

        def placed(table, green, sigma, phonon):
            green = pltpu.with_memory_space_constraint(green, pltpu.HBM)
            sigma = pltpu.with_memory_space_constraint(sigma, pltpu.VMEM)
            phonon = pltpu.with_memory_space_constraint(phonon, pltpu.HBM)
            table = pltpu.with_memory_space_constraint(table, pltpu.SMEM)
            return call(table, green, sigma, phonon)

        return placed

    sigma = sigma[0, 0].reshape(slots, 2, STRIPS, strip, width)
    phonon = phonon[0, 0].reshape(2, STRIPS, strip, width)
    arrays = (pair_off.T, pair_count, pair_range.T, sigma)
    which, table, sigma = pl.pallas_call(
        functools.partial(plan, slabs, strip, classes),
        out_shape=(
            pltpu.SMEM((1,), jnp.int32),
            pltpu.SMEM((slabs + 2, PAIRS + 2 * slots), jnp.int32),
            pltpu.VMEM(sigma.shape, sigma.dtype),
        ),
        in_specs=[hbm] * 4,
        out_specs=(smem, smem, vmem),
        scratch_shapes=[
            pltpu.SMEM((slots, slabs), jnp.int32),
            pltpu.SMEM((slabs,), jnp.int32),
            pltpu.SMEM((slots, slabs), jnp.int32),
            pltpu.SemaphoreType.DMA((3,)),
            pltpu.SemaphoreType.DMA((1,)),
        ],
        compiler_params=pltpu.CompilerParams(vmem_limit_bytes=GRANT),
    )(*[pltpu.with_memory_space_constraint(x, pltpu.HBM) for x in arrays])
    green = green[0, 0]
    result = lax.switch(
        which[0], [run(n) for n in range(len(classes))], table, green, sigma, phonon
    )
    return result[None, None]


def solution(mesh):
    in_specs = (
        P("energy", "slab", None, None, None, None),
        P("energy", "slab", None, None, None, None),
        P("energy", "slab", None, None, None),
        P(),
        P(),
        P(),
    )
    out_specs = P("energy", "slab", None, None, None)
    run = functools.partial(body, mesh.shape["slab"], mesh.shape["energy"])
    return jax.shard_map(run, mesh=mesh, in_specs=in_specs, out_specs=out_specs, check_vma=False)
```

```python
import functools

import jax
import jax.numpy as jnp
from jax import lax
from jax.experimental import pallas as pl
from jax.experimental.pallas import tpu as pltpu
from jax.sharding import PartitionSpec as P

STRIPS = 4
OFFSETS = (-2, -1, 1, 2)
LAG = 2
LENT = 4
PAIRS = 5
GRANT = 36 * 2**20
MESH = pl.DeviceIdType.MESH


def shapes(slots):
    most = STRIPS * min(slots, len(OFFSETS))
    reach = min(2 * STRIPS, most)
    sizes = ((4, 2), (5, 3), (5, 4), (6, 4), (6, 5), (7, 5), (7, 6), (8, 6))
    table = [(m, f, 4, min(2, m - 4), 2) for m, f in sizes]
    return [c for c in table if c[0] < most] + [(most, max(most - LAG, reach), 2, 0, 2)]


def plan(
    slabs,
    strip,
    classes,
    off_hbm,
    count_hbm,
    range_hbm,
    sigma_hbm,
    which_ref,
    plan_ref,
    sigma_v,
    off_ref,
    count_ref,
    range_ref,
    table_sem,
    load_sem,
):
    pairs = ((off_hbm, off_ref), (count_hbm, count_ref), (range_hbm, range_ref))
    tables = [pltpu.make_async_copy(a, b, table_sem.at[n]) for n, (a, b) in enumerate(pairs)]
    blocks = ((sigma_hbm, sigma_v),)
    fetches = [pltpu.make_async_copy(a, b, load_sem.at[n]) for n, (a, b) in enumerate(blocks)]
    for fetch in tables + fetches:
        fetch.start()
    for fetch in tables:
        fetch.wait()
    slots = off_ref.shape[0]
    levels = slabs // 2

    group = next(n for n in (4, 2, 1) if slabs % n == 0)

    def count(m, carry):
        for k in [m * group + n for n in range(group)]:
            side = 1 - 2 * lax.rem(k, 2)
            live_slots = count_ref[k]
            offsets, heights = [], []
            for q in range(slots):
                offset = jnp.where(q < live_slots, off_ref[q, k], 9)
                reach = range_ref[q, k]
                height = jnp.int32(0)
                for n in range(STRIPS):
                    height = jnp.where(reach > n * strip, n + 1, height)
                plan_ref[k, PAIRS + q] = offset
                plan_ref[k, PAIRS + slots + q] = reach
                offsets.append(offset * side)
                heights.append(height)
            for n, order in enumerate(OFFSETS):
                most = jnp.int32(0)
                for offset, height in zip(offsets, heights):
                    most = jnp.maximum(most, jnp.where(offset == order, height, 0))
                plan_ref[k, n] = most
        return carry

    lax.fori_loop(0, slabs // group, count, 0)
    plan_ref[slabs, LENT] = jnp.int32(0)

    chains = []
    for column in range(2):
        chain = [2 * p + 1 if column else slabs - 2 - 2 * p for p in range(levels)]
        far = [plan_ref[k, 0] + plan_ref[k, 1] for k in chain]
        near = [plan_ref[k, 2] + plan_ref[k, 3] for k in chain]
        chains.append((chain, far, near))

    def pick(table, n):
        value = jnp.int32(table[-1])
        for m, entry in enumerate(table[:-1]):
            value = jnp.where(n == m, entry, value)
        return value

    def attempt(state):
        n = state[0] + 1
        slots_y, forwarded, most_ahead, most_back, early = [pick(t, n) for t in zip(*classes)]
        free = slots_y - forwarded
        bad = jnp.int32(0)
        for chain, far, near in chains:
            moved = jnp.int32(0)
            for p, k in enumerate(chain):
                after = near[p + 1] if p + 1 < levels else 0
                behind = jnp.maximum(moved, 0)
                room = forwarded - early - jnp.maximum(behind - free, 0)
                need = jnp.maximum(near[p] + far[p] + moved - slots_y, far[p] - forwarded)
                pull = jnp.minimum(jnp.minimum(after, most_back), room)
                moved = jnp.maximum(need, -pull)
                bad = bad | jnp.where((moved > jnp.minimum(far[p], most_ahead)) | (room < 0), 1, 0)
                plan_ref[k, LENT] = moved
        return n, bad

    n, _ = lax.while_loop(lambda state: state[1] > 0, attempt, (jnp.int32(-1), jnp.int32(1)))
    which_ref[0] = n
    for fetch in fetches:
        fetch.wait()


def kernel(
    slabs,
    energies,
    cls,
    plan_ref,
    green_hbm,
    sigma_v,
    phonon_hbm,
    out_ref,
    green_v,
    own,
    inbox,
    ahead_box,
    back_box,
    sides,
    right,
    left,
    whole,
    total,
    inner,
    inner_strip,
    send_own,
    recv_own,
    send_far,
    recv_far,
    send_lent,
    recv_lent,
    send_side,
    recv_side,
    load_sem,
):
    slots_y, forwarded, lent_ahead, lent_back, early = cls
    free = slots_y - forwarded
    moves = slots_y + STRIPS
    passed = forwarded + STRIPS
    lent = lent_ahead + lent_back
    i = lax.axis_index("slab")
    e = lax.axis_index("energy")
    slots = sigma_v.shape[0]
    width = green_v.shape[-1]
    strip = width // STRIPS
    step = 1 - 2 * lax.rem(i, 2)
    partner = i + step
    goes = (i + 2 * step >= 0) & (i + 2 * step < slabs)
    comes = (i - 2 * step >= 0) & (i - 2 * step < slabs)
    onward = lax.rem(i + 2 * step + slabs, slabs)
    source = lax.rem(i - 2 * step + slabs, slabs)
    up = lax.rem(e + 1, energies)
    down = lax.rem(e - 1 + energies, energies)

    def remote(src, dst, send, recv, target):
        return pltpu.make_async_remote_copy(
            src_ref=src,
            dst_ref=dst,
            send_sem=send,
            recv_sem=recv,
            device_id=target,
            device_id_type=MESH,
        )

    def own_copy(n):
        return remote(own.at[n], inbox.at[n], send_own.at[n], recv_own.at[n], {"slab": partner})

    def far_copy(n):
        return remote(
            inbox.at[n], inbox.at[moves + n], send_far.at[n], recv_far.at[n], {"slab": onward}
        )

    def ahead_copy(n):
        return remote(
            own.at[moves + n], ahead_box.at[n], send_lent.at[n], recv_lent.at[n], {"slab": source}
        )

    def back_copy(n):
        return remote(
            own.at[moves + lent_ahead + n],
            back_box.at[n],
            send_lent.at[lent_ahead + n],
            recv_lent.at[lent_ahead + n],
            {"slab": onward},
        )

    def side_copy(place, s, target):
        return remote(
            phonon_hbm.at[:, s],
            sides.at[place, s],
            send_side.at[place, s],
            recv_side.at[place, s],
            {"energy": target},
        )

    load = pltpu.make_async_copy(green_hbm, green_v, load_sem)
    load.start()

    barrier = pltpu.get_barrier_semaphore()
    for target in (partner, onward, source):
        pl.semaphore_signal(barrier, inc=1, device_id={"slab": target}, device_id_type=MESH)
    for target in (up, down):
        pl.semaphore_signal(barrier, inc=1, device_id={"energy": target}, device_id_type=MESH)

    rows = lax.broadcasted_iota(jnp.int32, (strip, width), 0)
    cols = lax.broadcasted_iota(jnp.int32, (strip, width), 1)

    def item(k, t):
        side = 1 - 2 * lax.rem(k, 2)
        first = plan_ref[k, 0]
        second = first + plan_ref[k, 1]
        third = second + plan_ref[k, 2]
        offset = jnp.where(t < first, -2, jnp.where(t < second, -1, jnp.where(t < third, 1, 2)))
        base = jnp.where(
            t < first, 0, jnp.where(t < second, first, jnp.where(t < third, second, third))
        )
        return offset * side, jnp.clip(t - base, 0, STRIPS - 1)

    def lending(k):
        before = k + 2 - 4 * lax.rem(k, 2)
        before = jnp.where((before >= 0) & (before < slabs), before, slabs)
        gives, takes = plan_ref[k, LENT], plan_ref[before, LENT]
        return (
            jnp.maximum(gives, 0),
            jnp.maximum(-takes, 0),
            jnp.maximum(takes, 0),
            jnp.maximum(-gives, 0),
        )

    def slot(k, j):
        far = plan_ref[k, 0] + plan_ref[k, 1]
        near = plan_ref[k, 2] + plan_ref[k, 3]
        lent_far, lent_near, behind, ahead = lending(k)
        far_own = far - lent_far
        near_own = near - lent_near
        behind_late = jnp.minimum(behind, free)
        near_late = jnp.minimum(near_own, free - behind_late)
        behind_first = behind - behind_late
        near_first = near_own - near_late
        ahead_at = forwarded - ahead
        behind_at = ahead_at - behind_first
        u = j - forwarded
        kind = jnp.int32(0)
        entry = jnp.int32(0)
        for here, what, value in (
            ((u < 0) & (j < far_own + near_first), 2, far + j - far_own),
            ((u < 0) & (j < far_own), 1, j),
            ((u < 0) & (j >= behind_at), 3, j - behind_at),
            ((u < 0) & (j >= ahead_at), 4, j - ahead_at),
            ((u >= 0) & (u < near_late + behind_late), 3, behind_first + u - near_late),
            ((u >= 0) & (u < near_late), 2, far + near_first + u),
        ):
            kind = jnp.where(here, what, kind)
            entry = jnp.where(here, value, entry)
        return kind, entry

    def merged(offset, at_row, part, value):
        furthest = jnp.maximum(rows + at_row * strip, cols)
        for q in range(slots):
            used = plan_ref[i, PAIRS + q] == offset
            reach = jnp.where(used, plan_ref[i, PAIRS + slots + q], 0)
            value += jnp.where(furthest < reach, sigma_v[q, part, at_row].astype(jnp.float32), 0.0)
        return value.astype(jnp.bfloat16)

    def fresh(offset, at_row, part):
        return merged(offset, at_row, part, jnp.zeros((strip, width), jnp.float32))

    def pack_first(t, carry):
        head = min(2, early)
        is_lent = (t >= head) & (t < head + lent)
        j = jnp.where(t < head, t, t - lent)
        kind, entry = slot(i, j)
        far = plan_ref[i, 0] + plan_ref[i, 1]
        given = t - head
        back = given - lent_ahead
        near = plan_ref[i, 2] + plan_ref[i, 3]
        lent_far, lent_near, _, _ = lending(i)
        lent_entry = jnp.where(back >= 0, far + near - lent_near + back, far - lent_far + given)
        lent_live = jnp.where(back >= 0, back < lent_near, given < lent_far)
        entry = jnp.where(is_lent, lent_entry, entry)
        live = (is_lent & lent_live) | (jnp.logical_not(is_lent) & ((kind == 1) | (kind == 2)))
        offset, at_row = item(i, entry)
        offset = jnp.where(live, offset, 8)
        into = jnp.where(is_lent, moves + given, j)

        def one(part, inside):
            own[into, part] = fresh(offset, at_row, part)
            return inside

        lax.fori_loop(0, 2, one, 0)

        @pl.when(t == 0)
        def _():
            pl.semaphore_wait(barrier, 5)

        @pl.when(jnp.logical_not(is_lent))
        def _():
            own_copy(j).start()

        @pl.when(is_lent & (back < 0) & comes)
        def _():
            ahead_copy(given).start()

        if lent_back:

            @pl.when(is_lent & (back >= 0) & goes)
            def _():
                back_copy(back).start()

        @pl.when(t == 0)
        def _():
            for s in range(STRIPS):

                @pl.when(e < energies - 1)
                def _():
                    side_copy(0, s, up).start()

                @pl.when(e > 0)
                def _():
                    side_copy(1, s, down).start()

        return carry

    lax.fori_loop(0, early + lent, pack_first, 0)

    def pack_late():
        @pl.when(goes)
        def _():
            for n in range(lent_ahead):
                ahead_copy(n).wait_recv()

        if lent_back:

            @pl.when(comes)
            def _():
                for n in range(lent_back):
                    back_copy(n).wait_recv()

        def one(j, carry):
            kind, entry = slot(i, j)
            offset, at_row = item(i, entry)
            offset = jnp.where((kind == 1) | (kind == 2), offset, 8)

            def half(part, inside):
                value = fresh(offset, at_row, part)
                value = jnp.where(
                    kind == 3, ahead_box[jnp.clip(entry, 0, lent_ahead - 1), part], value
                )
                if lent_back:
                    value = jnp.where(
                        kind == 4, back_box[jnp.clip(entry, 0, lent_back - 1), part], value
                    )
                own[j + STRIPS, part] = value
                return inside

            lax.fori_loop(0, 2, half, 0)
            own_copy(j + STRIPS).start()
            return carry

        lax.fori_loop(early, slots_y, one, 0)

    def pass_on(n):
        own_copy(n).wait_recv()

        @pl.when(goes & (n < passed))
        def _():
            far_copy(n).start()

    load.wait()

    def arrange(place, carry):
        real = green_v[place, 0]
        imag = green_v[place, 1]
        for g in range(STRIPS):
            span = slice(g * strip, (g + 1) * strip)
            left[place, g] = jnp.concatenate([real[:, span], imag[:, span]], axis=1)
        real_t = real.T
        imag_t = imag.T
        right[place, :width, :width] = real_t
        right[place, width:, :width] = imag_t
        right[place, :width, width:] = -imag_t
        right[place, width:, width:] = real_t
        return carry

    lax.fori_loop(0, 3, arrange, 0)

    tile = 2 * width // 3

    def multiply(place):
        def one(n, carry):
            span = pl.ds(pl.multiple_of(n * tile, tile), tile)
            total[:, span] += jnp.dot(
                whole[...], right[place, :, span], preferred_element_type=jnp.float32
            )
            return carry

        lax.fori_loop(0, 3, one, 0)

    total[...] = jnp.zeros_like(total)

    def add_own(m, carry):
        for s in range(STRIPS):
            for part in range(2):
                whole[s * strip : (s + 1) * strip, part * width : (part + 1) * width] = fresh(
                    2 * m - 1, s, part
                )
        multiply(2 * m)
        return carry

    lax.fori_loop(0, 2, add_own, 0)

    def mix(s, carry):
        @pl.when(e > 0)
        def _():
            side_copy(0, s, up).wait_recv()

        @pl.when(e == 0)
        def _():
            sides[0, s] = jnp.zeros(sides.shape[2:], sides.dtype)

        @pl.when(e < energies - 1)
        def _():
            side_copy(1, s, down).wait_recv()

        @pl.when(e == energies - 1)
        def _():
            sides[1, s] = jnp.zeros(sides.shape[2:], sides.dtype)

        for part in range(2):
            mixed = 0.5 * (
                sides[0, s, part].astype(jnp.float32) + sides[1, s, part].astype(jnp.float32)
            )
            mixed = mixed.astype(jnp.bfloat16).astype(jnp.float32)
            own[early + s, part] = merged(0, s, part, mixed)
        own_copy(early + s).start()

        @pl.when(s == 0)
        def _():
            pass_on(0)

        @pl.when(s == STRIPS - 2)
        def _():
            pass_on(1)

        return carry

    lax.fori_loop(0, STRIPS, mix, 0)

    for s in range(STRIPS):
        for part in range(2):
            whole[s * strip : (s + 1) * strip, part * width : (part + 1) * width] = own[
                early + s, part
            ]
    multiply(1)
    mine = total[...].astype(jnp.bfloat16)
    inner[:width, :] = mine
    inner[width:, :width] = -mine[:, width:]
    inner[width:, width:] = mine[:, :width]
    both = jnp.concatenate([green_v[1, 0], green_v[1, 1]], axis=1)
    for part in range(2):
        out_ref[part] = jnp.dot(
            both, inner[:, part * width : (part + 1) * width], preferred_element_type=jnp.float32
        )

    other = i - step

    def handle(at, n, across):
        j = jnp.where(n < early, n, n - STRIPS)
        middle = (n >= early) & (n < early + STRIPS)
        k = jnp.clip(jnp.where(across, partner, other), 0, slabs - 1)
        kind, entry = slot(k, j)
        crossed = kind == jnp.where(across, 3, 4)
        direct = kind == jnp.where(across, 2, 1)
        k_from = jnp.clip(jnp.where(across, other, partner), 0, slabs - 1)
        far_from = plan_ref[k_from, 0] + plan_ref[k_from, 1]
        near_from = plan_ref[k_from, 2] + plan_ref[k_from, 3]
        lent_far, lent_near, _, _ = lending(k_from)
        entry_from = entry + jnp.where(
            across, far_from - lent_far, far_from + near_from - lent_near
        )
        k_used = jnp.where(crossed & jnp.logical_not(middle), k_from, k)
        offset, at_row = item(k_used, jnp.where(crossed, entry_from, entry))
        offset = jnp.where(middle, 0, offset)
        at_row = jnp.where(middle, jnp.clip(n - early, 0, STRIPS - 1), at_row)
        valid = middle | crossed | direct
        place = jnp.clip(k_used + offset - i + 1, 0, 2)
        column = jnp.clip(k_used - i + 1, 0, 2)
        data = jnp.concatenate([inbox[at, 0], inbox[at, 1]], axis=1)
        value = jnp.dot(data, right[place], preferred_element_type=jnp.float32)
        value = jnp.where(valid, value, 0.0).astype(jnp.bfloat16)
        inner_strip[:strip, :] = value
        inner_strip[strip:, :width] = -value[:, width:]
        inner_strip[strip:, width:] = value[:, :width]
        for part in range(2):
            out_ref[part] += jnp.dot(
                left[column, at_row],
                inner_strip[:, part * width : (part + 1) * width],
                preferred_element_type=jnp.float32,
            )

    def event(t, carry):
        n = t // 2
        across = lax.rem(t, 2) == 1
        m = n - LAG

        @pl.when(across & (n >= 2))
        def _():
            pass_on(n)

        @pl.when(across & (n == 3))
        def _():
            pack_late()

        @pl.when(jnp.logical_not(across) & (m >= 0) & comes)
        def _():
            far_copy(m).wait_recv()

        @pl.when(across | ((m >= 0) & comes))
        def _():
            index = jnp.where(across, n, m)
            handle(jnp.where(across, n, jnp.maximum(moves + m, 0)), index, across)

        return carry

    lax.fori_loop(0, 2 * moves, event, 0)

    for n in range(moves - LAG, passed):

        @pl.when(comes)
        def _():
            far_copy(n).wait_recv()
            handle(moves + n, jnp.int32(n), jnp.bool_(False))

    def sent(n, carry):
        own_copy(n).wait_send()

        @pl.when(goes & (n < passed))
        def _():
            far_copy(n).wait_send()

        return carry

    lax.fori_loop(0, moves, sent, 0)

    @pl.when(comes)
    def _():
        for n in range(lent_ahead):
            ahead_copy(n).wait_send()

    if lent_back:

        @pl.when(goes)
        def _():
            for n in range(lent_back):
                back_copy(n).wait_send()

    for s in range(STRIPS):

        @pl.when(e < energies - 1)
        def _():
            side_copy(0, s, up).wait_send()

        @pl.when(e > 0)
        def _():
            side_copy(1, s, down).wait_send()


def body(slabs, energies, green, sigma, phonon, pair_off, pair_count, pair_range):
    width = green.shape[-1]
    slots = sigma.shape[2]
    strip = width // STRIPS
    hbm = pl.BlockSpec(memory_space=pl.ANY)
    smem = pl.BlockSpec(memory_space=pltpu.SMEM)
    vmem = pl.BlockSpec(memory_space=pltpu.VMEM)
    classes = shapes(slots)
    block = (2, width, width)
    cut = (2, strip, width)

    def run(n):
        cls = classes[n]
        slots_y, forwarded, lent_ahead, lent_back, _ = cls
        moves = slots_y + STRIPS
        passed = forwarded + STRIPS
        lent = lent_ahead + lent_back
        call = pl.pallas_call(
            functools.partial(kernel, slabs, energies, cls),
            out_shape=jax.ShapeDtypeStruct(block, jnp.float32),
            in_specs=[smem, hbm, vmem, hbm],
            out_specs=vmem,
            scratch_shapes=[
                pltpu.VMEM((3,) + block, jnp.bfloat16),
                pltpu.VMEM((moves + lent,) + cut, jnp.bfloat16),
                pltpu.VMEM((moves + passed,) + cut, jnp.bfloat16),
                pltpu.VMEM((lent_ahead,) + cut, jnp.bfloat16),
                pltpu.VMEM((max(1, lent_back),) + cut, jnp.bfloat16),
                pltpu.VMEM((2, STRIPS) + cut, jnp.bfloat16),
                pltpu.VMEM((3, 2 * width, 2 * width), jnp.bfloat16),
                pltpu.VMEM((3, STRIPS, width, 2 * strip), jnp.bfloat16),
                pltpu.VMEM((width, 2 * width), jnp.bfloat16),
                pltpu.VMEM((width, 2 * width), jnp.float32),
                pltpu.VMEM((2 * width, 2 * width), jnp.bfloat16),
                pltpu.VMEM((2 * strip, 2 * width), jnp.bfloat16),
                pltpu.SemaphoreType.DMA((moves,)),
                pltpu.SemaphoreType.DMA((moves,)),
                pltpu.SemaphoreType.DMA((passed,)),
                pltpu.SemaphoreType.DMA((passed,)),
                pltpu.SemaphoreType.DMA((lent,)),
                pltpu.SemaphoreType.DMA((lent,)),
                pltpu.SemaphoreType.DMA((2, STRIPS)),
                pltpu.SemaphoreType.DMA((2, STRIPS)),
                pltpu.SemaphoreType.DMA,
            ],
            compiler_params=pltpu.CompilerParams(
                collective_id=n, has_side_effects=True, vmem_limit_bytes=GRANT
            ),
        )

        def placed(table, green, sigma, phonon):
            green = pltpu.with_memory_space_constraint(green, pltpu.HBM)
            sigma = pltpu.with_memory_space_constraint(sigma, pltpu.VMEM)
            phonon = pltpu.with_memory_space_constraint(phonon, pltpu.HBM)
            table = pltpu.with_memory_space_constraint(table, pltpu.SMEM)
            return call(table, green, sigma, phonon)

        return placed

    sigma = sigma[0, 0].reshape(slots, 2, STRIPS, strip, width)
    phonon = phonon[0, 0].reshape(2, STRIPS, strip, width)
    arrays = (pair_off.T, pair_count, pair_range.T, sigma)
    which, table, sigma = pl.pallas_call(
        functools.partial(plan, slabs, strip, classes),
        out_shape=(
            pltpu.SMEM((1,), jnp.int32),
            pltpu.SMEM((slabs + 2, PAIRS + 2 * slots), jnp.int32),
            pltpu.VMEM(sigma.shape, sigma.dtype),
        ),
        in_specs=[hbm] * 4,
        out_specs=(smem, smem, vmem),
        scratch_shapes=[
            pltpu.SMEM((slots, slabs), jnp.int32),
            pltpu.SMEM((slabs,), jnp.int32),
            pltpu.SMEM((slots, slabs), jnp.int32),
            pltpu.SemaphoreType.DMA((3,)),
            pltpu.SemaphoreType.DMA((1,)),
        ],
        compiler_params=pltpu.CompilerParams(vmem_limit_bytes=GRANT),
    )(*[pltpu.with_memory_space_constraint(x, pltpu.HBM) for x in arrays])
    green = green[0, 0]
    result = lax.switch(
        which[0], [run(n) for n in range(len(classes))], table, green, sigma, phonon
    )
    return result[None, None]


def solution(mesh):
    in_specs = (
        P("energy", "slab", None, None, None, None),
        P("energy", "slab", None, None, None, None),
        P("energy", "slab", None, None, None),
        P(),
        P(),
        P(),
    )
    out_specs = P("energy", "slab", None, None, None)
    run = functools.partial(body, mesh.shape["slab"], mesh.shape["energy"])
    return jax.shard_map(run, mesh=mesh, in_specs=in_specs, out_specs=out_specs, check_vma=False)
```
